32 devices in a mesh: param: 8 (over z, y), sensor: 4 (over x, core).
Axes of the slice: x: 2, y: 2, z: 4, core: 2. Of those that a mesh axis runs over, the one named last changes fastest.
Arguments:
- blocks: bfloat16 [64, 2, 600, 1024], P(None, None, 'sensor', 'param'), may hold values from -0.1875 to 0.1875
- probes: bfloat16 [64, 2, 4, 1024], P(None, None, None, 'param'), may hold values from -6 to 6
Outputs:
- basis: float32 [64, 2, 4, 600], P(None, None, None, 'sensor')
- coeffs: bfloat16 [64, 2, 4, 1024], P('sensor', None, None, 'param')
The draws below stay inside these ranges and needn't reach their ends.
All inputs are finite; a program needn't handle non-finite values.
Results may differ from the reference program's by a relative error of at most 0.0049.
Values sent between devices are 32-bit elements; how exact they have to be, the bound alone decides.
No kernel may reach another device: no remote copies, remote signals or barrier semaphores. Data moves between devices by JAX's collectives and lax.ppermute only.
A program may use at most 64 MiB of HBM per device.

```python
import jax
import jax.numpy as jnp
from jax import lax

SENSORS = 600
FREQ_LINES = 64
PROBES = 4
NODES = 1024


def steps_of(own_key, dims, cuts, least, largest):
    loudness = 1.0
    for axis_at, shards_of in cuts:
        draws = jax.random.uniform(jax.random.fold_in(jax.random.fold_in(own_key, 6), axis_at), (shards_of,), jnp.float32, least / len(cuts), largest / len(cuts))
        loudness = loudness * jnp.repeat(jnp.exp(draws), dims[axis_at] // shards_of).reshape((-1,) + (1,) * (len(dims) - 1 - axis_at))
    return loudness


def scatter_about(stream_key, dims, deviation, limit, cuts=(), kind=jnp.bfloat16):
    gain = steps_of(stream_key, dims, cuts, -0.22, 0.18) if cuts else 1.0
    entries = jax.random.normal(stream_key, dims, jnp.float32) * deviation * gain
    return jnp.minimum(jnp.maximum(entries, -limit), limit).astype(kind)


def setup_inputs(seed: int = 0) -> dict:
    key_list = jax.random.split(jax.random.key(seed), 3)
    blocks = scatter_about(key_list[0], (FREQ_LINES, 2, SENSORS, NODES), (2 * SENSORS) ** -0.5, 0.1875, ((2, 4), (3, 8)))
    probes = scatter_about(key_list[1], (FREQ_LINES, 2, PROBES, NODES), 1.0, 6.0, ((3, 8),))
    return {"blocks": blocks, "probes": probes}


def sketch_line(pair):
    block, probe = pair
    block = block.astype(jnp.float32)
    probe = probe.astype(jnp.float32)
    real_part = jnp.einsum('sn,an->as', block[0], probe[0]) - jnp.einsum('sn,an->as', block[1], probe[1])
    imag_part = jnp.einsum('sn,an->as', block[0], probe[1]) + jnp.einsum('sn,an->as', block[1], probe[0])
    return jnp.stack([real_part, imag_part])

def adjoint_line(pair):
    block, vectors = pair
    block = block.astype(jnp.float32)
    vectors = vectors.astype(jnp.float32)
    real_part = jnp.einsum('sn,as->an', block[0], vectors[0]) + jnp.einsum('sn,as->an', block[1], vectors[1])
    imag_part = jnp.einsum('sn,as->an', block[0], vectors[1]) - jnp.einsum('sn,as->an', block[1], vectors[0])
    return jnp.stack([real_part, imag_part])

def reference(blocks, probes):
    sketch = lax.map(sketch_line, (blocks, probes))
    gram = jnp.einsum('fpas,fpbs->ab', sketch, sketch, precision=lax.Precision.HIGHEST) / (2.0 * FREQ_LINES * SENSORS)
    lower = jnp.linalg.cholesky(gram)
    inverse = lax.linalg.triangular_solve(lower, jnp.eye(PROBES, dtype=gram.dtype), left_side=True, lower=True)
    basis = jnp.einsum('ab,fpbs->fpas', inverse, sketch, precision=lax.Precision.HIGHEST)
    rounded = lax.optimization_barrier(basis.astype(jnp.bfloat16))
    coeffs = lax.map(adjoint_line, (blocks, rounded))
    return (basis, coeffs.astype(jnp.bfloat16))
```

```python
import functools

import jax
import jax.numpy as jnp
from jax import lax
from jax.experimental import pallas as pl
from jax.experimental.pallas import tpu as pltpu
from jax.sharding import PartitionSpec as P

LANES = 128
STEP = 2 * LANES
QUAD = 4
PROBES = 4
SPLITS = 3


def roll(x, shift, axis):
    return pltpu.roll(x, shift % x.shape[axis], axis)


def row_of(shape=(8, LANES)):
    return lax.broadcasted_iota(jnp.int32, shape, 0)


def lane_of(shape=(8, LANES)):
    return lax.broadcasted_iota(jnp.int32, shape, 1)


class Plan:
    def __init__(self, lines, parts, group, nodes, shards):
        self.lines, self.parts, self.group, self.nodes = lines, parts, group, nodes
        self.per_line = parts * group
        self.rows = lines * self.per_line
        self.steps = self.rows // STEP
        self.quarter = -(-self.steps // QUAD)
        self.shards = shards
        self.shard_lines = lines // shards
        self.total = parts * lines * group * shards
        assert parts == 2 and nodes == LANES and self.rows % STEP == 0 and self.per_line >= STEP
        assert lines % shards == 0 and self.steps > (QUAD - 1) * self.quarter


def first_line(plan, step):
    return (step * STEP) // plan.per_line


def sketch_kernel(plan, me_ref, blocks_ref, probes_ref, *rest):
    outs, kept_ref, lhs_ref, sems = rest[:QUAD], rest[QUAD], rest[QUAD + 1], rest[QUAD + 2]
    me = me_ref[0]
    main = plan.quarter - 1
    order = [k for k in range(1, QUAD)] + [0]

    def copies(k):
        first = (me ^ k) * plan.quarter
        tail = jnp.minimum(first + main, plan.steps - 1)
        return (
            pltpu.make_async_copy(
                blocks_ref.at[pl.ds(pl.multiple_of(first * STEP, STEP), main * STEP)],
                kept_ref.at[k, pl.ds(0, main * STEP)],
                sems.at[k, 0],
            ),
            pltpu.make_async_copy(
                blocks_ref.at[pl.ds(pl.multiple_of(tail * STEP, STEP), STEP)],
                kept_ref.at[k, pl.ds(main * STEP, STEP)],
                sems.at[k, 1],
            ),
        )

    for k in order:
        for copy in copies(k):
            copy.start()
    held = plan.lines * 2 * PROBES
    lhs_ref[pl.ds(0, held)] = probes_ref[...].astype(jnp.float32)
    lhs_ref[pl.ds(held, 8)] = jnp.zeros((8, LANES), jnp.float32)
    low = row_of() < 4
    even = lane_of() % 2 == 0
    column = lane_of((8, STEP))
    for k in order:
        for copy in copies(k):
            copy.wait()
        first = (me ^ k) * plan.quarter

        def body(t, _, k=k, first=first):
            step = first + t
            line = first_line(plan, jnp.minimum(step, plan.steps - 1))
            probe = lhs_ref[pl.ds(pl.multiple_of(line * 8, 8), 16)].astype(jnp.bfloat16)
            block = kept_ref[k, pl.ds(pl.multiple_of(t * STEP, STEP), STEP)]
            both = lax.dot_general(probe, block, (((1,), (1,)), ((), ())), preferred_element_type=jnp.float32)
            place = column + step * STEP
            own = jnp.where(place < (line + 1) * plan.per_line, both[:8], both[8:])
            own = jnp.where(place < plan.rows, own, 0.0)
            left, right = own[:, :LANES], own[:, LANES:]
            direct = jnp.where(low, left, roll(right, 4, 0))
            crossed = jnp.where(low, roll(left, 4, 0), right)
            outs[k][t] = direct + jnp.where(even, -roll(crossed, -1, 1), roll(crossed, 1, 1))
            return 0

        lax.fori_loop(0, plan.quarter, body, 0, unroll=True)


def sketch_terms(plan, me, blocks, probes):
    piece = jax.ShapeDtypeStruct((plan.quarter, 8, LANES), jnp.float32)
    kept = jax.ShapeDtypeStruct((QUAD, plan.quarter * STEP, LANES), jnp.bfloat16)
    vmem = pl.BlockSpec(memory_space=pltpu.VMEM)
    out = pl.pallas_call(
        functools.partial(sketch_kernel, plan),
        out_shape=[piece] * QUAD + [kept],
        in_specs=[pl.BlockSpec(memory_space=pltpu.SMEM), pl.BlockSpec(memory_space=pl.ANY), vmem],
        out_specs=[vmem] * (QUAD + 1),
        scratch_shapes=[
            pltpu.VMEM((plan.lines * 8 + 8, LANES), jnp.float32),
            pltpu.SemaphoreType.DMA((QUAD, 2)),
        ],
        name="sketch_terms",
    )(me, blocks, probes)
    return out[:QUAD], out[QUAD]


def gram_kernel(plan, *refs):
    ins, out_ref = refs[:-1], refs[-1]
    row = row_of()
    lane = lane_of()
    sums = [jnp.zeros((8, LANES), jnp.float32) for _ in range(3)]
    for t in range(plan.quarter):
        x = ins[0][t]
        for other in ins[1:]:
            x = x + other[t]
        out_ref[t] = x
        for d in range(3):
            y = x if d == 0 else jnp.where(row % 4 + d < 4, roll(x, -d, 0), roll(x, 4 - d, 0))
            sums[d] = sums[d] + x * y
    packed = jnp.zeros((8, LANES), jnp.float32)
    for d in range(3):
        packed = jnp.where(lane == d, jnp.sum(sums[d], axis=1, keepdims=True), packed)
    out_ref[plan.quarter] = packed


def add_with_gram(plan, *pieces):
    vmem = pl.BlockSpec(memory_space=pltpu.VMEM)
    return pl.pallas_call(
        functools.partial(gram_kernel, plan),
        out_shape=jax.ShapeDtypeStruct((plan.quarter + 1, 8, LANES), jnp.float32),
        in_specs=[vmem] * len(pieces),
        out_specs=vmem,
        name="add_with_gram",
    )(*pieces)


def adjoint_kernel(plan, me_ref, spot_ref, kept_ref, *rest):
    ins, outs, acc_ref = rest[:QUAD], rest[QUAD : QUAD + plan.shards], rest[QUAD + plan.shards]
    me = me_ref[0]
    spot = spot_ref[0]
    low = row_of() < 4
    even = lane_of() % 2 == 0
    column = lane_of((8, STEP))
    acc_ref[...] = jnp.zeros(acc_ref.shape, jnp.float32)
    for k in range(QUAD):
        first = (me ^ k) * plan.quarter

        def body(t, _, k=k, first=first):
            step = jnp.minimum(first + t, plan.steps - 1)
            line = first_line(plan, step)
            x = ins[k][t]
            y = jnp.where(even, roll(x, -1, 1), -roll(x, 1, 1))
            left = jnp.where(low, x, roll(y, 4, 0))
            right = jnp.where(low, roll(x, 4, 0), y)
            value = jnp.concatenate([left, right], axis=1)
            mine = column + step * STEP < (line + 1) * plan.per_line
            terms = []
            for _ in range(SPLITS):
                term = value.astype(jnp.bfloat16).astype(jnp.float32)
                terms.append(jnp.where(mine, term, 0.0))
                terms.append(jnp.where(mine, 0.0, term))
                value = value - term
            lhs = jnp.concatenate(terms, axis=0).astype(jnp.bfloat16)
            block = kept_ref[k, pl.ds(pl.multiple_of(t * STEP, STEP), STEP)]
            got = jnp.dot(lhs, block, preferred_element_type=jnp.float32)
            here = sum(got[16 * i : 16 * i + 8] for i in range(SPLITS))
            after = sum(got[16 * i + 8 : 16 * i + 16] for i in range(SPLITS))
            acc_ref[line] = acc_ref[line] + here
            acc_ref[line + 1] = acc_ref[line + 1] + after
            return 0

        lax.fori_loop(0, plan.quarter, body, 0, unroll=True)
    packed = sum(ref[plan.quarter] for ref in ins)
    for k in range(plan.shards):
        start = (spot ^ k) * plan.shard_lines
        outs[k][pl.ds(0, plan.shard_lines)] = acc_ref[pl.ds(start, plan.shard_lines)]
        outs[k][plan.shard_lines] = packed


def adjoint_terms(plan, me, spot, kept, pieces):
    vmem = pl.BlockSpec(memory_space=pltpu.VMEM)
    smem = pl.BlockSpec(memory_space=pltpu.SMEM)
    return pl.pallas_call(
        functools.partial(adjoint_kernel, plan),
        out_shape=[jax.ShapeDtypeStruct((plan.shard_lines + 1, 8, LANES), jnp.float32)] * plan.shards,
        in_specs=[smem, smem] + [vmem] * (1 + QUAD),
        out_specs=[vmem] * plan.shards,
        scratch_shapes=[pltpu.VMEM((plan.lines + 1, 8, LANES), jnp.float32)],
        name="adjoint_terms",
    )(me, spot, kept, *pieces)


def by_line_kernel(plan, me_ref, *rest):
    ins, out_ref, flat_ref = rest[:QUAD], rest[QUAD], rest[QUAD + 1]
    me = me_ref[0]
    lane = lane_of()
    half = LANES // 2
    stay = (row_of() < 4) == (lane < half)
    source = jnp.where(lane < half, 2 * lane, 2 * lane - (LANES - 1))
    for k in range(QUAD):
        first = (me ^ k) * plan.quarter
        for t in range(plan.quarter):
            split = jnp.take_along_axis(ins[k][t], source, axis=1)
            flat_ref[first + t] = jnp.where(stay, split, roll(roll(split, 4, 0), half, 1))
    tiles = -(-plan.group // LANES)
    for line in range(plan.lines):
        tile, shift = divmod(line * plan.group, LANES)
        turned = [roll(flat_ref[tile + i], -shift, 1) for i in range(tiles + 1)]
        for i in range(tiles):
            width = min(LANES, plan.group - i * LANES)
            part = jnp.where(lane < LANES - shift, turned[i], turned[i + 1])
            out_ref[line, :, pl.ds(i * LANES, width)] = part[:, :width]


def sketch_by_line(plan, me, pieces):
    vmem = pl.BlockSpec(memory_space=pltpu.VMEM)
    return pl.pallas_call(
        functools.partial(by_line_kernel, plan),
        out_shape=jax.ShapeDtypeStruct((plan.lines, 8, plan.group), jnp.float32),
        in_specs=[pl.BlockSpec(memory_space=pltpu.SMEM)] + [vmem] * QUAD,
        out_specs=vmem,
        scratch_shapes=[pltpu.VMEM((QUAD * plan.quarter + 2, 8, LANES), jnp.float32)],
        name="sketch_by_line",
    )(me, *pieces)


def inverse_rows(plan, packed):
    row = row_of()
    lane = lane_of()
    packed = packed + roll(packed, 4, 0)
    entry = {}
    for d in range(3):
        for a in range(PROBES):
            b = (a + d) % PROBES
            if (max(a, b), min(a, b)) not in entry:
                chosen = jnp.where((row == a) & (lane == d), packed, 0.0)
                whole = jnp.sum(jnp.sum(chosen, axis=1, keepdims=True), axis=0, keepdims=True)
                entry[max(a, b), min(a, b)] = jnp.broadcast_to(whole, (8, LANES)) / plan.total
    low = {}
    inv = {}
    for j in range(PROBES):
        rest = entry[j, j]
        for m in range(j):
            rest = rest - low[j, m] * low[j, m]
        low[j, j] = jnp.sqrt(rest)
        inv[j, j] = 1.0 / low[j, j]
        for i in range(j + 1, PROBES):
            rest = entry[i, j]
            for m in range(j):
                rest = rest - low[i, m] * low[j, m]
            low[i, j] = rest * inv[j, j]
    for i in range(PROBES):
        for j in range(i):
            total = sum(low[i, m] * inv[m, j] for m in range(j, i))
            inv[i, j] = -total * inv[i, i]
    rows = []
    for d in range(PROBES):
        value = jnp.zeros((8, LANES), jnp.float32)
        for a in range(d, PROBES):
            value = jnp.where(row % 4 == a, inv[a, a - d], value)
        rows.append(value)
    return rows


def final_kernel(plan, sketch_ref, *rest):
    ins, basis_ref, coeffs_ref = rest[: plan.shards], rest[plan.shards], rest[plan.shards + 1]
    packed = sum(ref[plan.shard_lines] for ref in ins)
    rows = inverse_rows(plan, packed)

    def scaled(x):
        width = x.shape[1]
        return sum((rows[d][:, :width] * (roll(x, d, 0) if d else x)) for d in range(PROBES))

    for pair in range(plan.shard_lines // 2):
        two = [scaled(sum(ref[2 * pair + i] for ref in ins)) for i in range(2)]
        coeffs_ref[pl.ds(16 * pair, 16)] = jnp.concatenate(two, axis=0).astype(jnp.bfloat16)
    for line in range(plan.lines):
        for start in range(0, plan.group, LANES):
            width = min(LANES, plan.group - start)
            value = scaled(sketch_ref[line, :, pl.ds(start, width)])
            for part in range(2):
                basis_ref[line, part, :, pl.ds(start, width)] = value[4 * part : 4 * part + 4]


def finish(plan, sketch, pieces):
    vmem = pl.BlockSpec(memory_space=pltpu.VMEM)
    return pl.pallas_call(
        functools.partial(final_kernel, plan),
        out_shape=[
            jax.ShapeDtypeStruct((plan.lines, 2, PROBES, plan.group), jnp.float32),
            jax.ShapeDtypeStruct((plan.shard_lines * 8, LANES), jnp.bfloat16),
        ],
        in_specs=[vmem] * (1 + plan.shards),
        out_specs=[vmem] * 2,
        name="finish",
    )(sketch, *pieces)


def trade(x, axis, size, k):
    return lax.ppermute(x, axis, [(i, i ^ k) for i in range(size)])


def on_device(param, sensor, blocks, probes):
    lines, parts, group, nodes = blocks.shape
    plan = Plan(lines, parts, group, nodes, sensor)
    rank = lax.axis_index("param")
    me = (rank % QUAD).astype(jnp.int32).reshape(1)
    spot = lax.axis_index("sensor").astype(jnp.int32).reshape(1)
    flat_blocks = blocks.transpose(0, 2, 1, 3).reshape(plan.rows, nodes)
    flat_probes = probes.reshape(lines * parts * PROBES, nodes)
    terms, kept = sketch_terms(plan, me, flat_blocks, flat_probes)
    total = terms[0] + sum(trade(terms[k], "param", param, k) for k in range(1, QUAD))
    span = QUAD
    while span * 2 < param:
        total = total + trade(total, "param", param, span)
        span *= 2
    sums = [total] + ([trade(total, "param", param, span)] if span < param else [])
    own = add_with_gram(plan, *sums)
    pieces = [own] + [trade(own, "param", param, k) for k in range(1, QUAD)]
    adjoint = adjoint_terms(plan, me, spot, kept, pieces)
    gathered = [adjoint[0]] + [trade(adjoint[k], "sensor", sensor, k) for k in range(1, sensor)]
    sketch = sketch_by_line(plan, me, pieces)
    basis, coeffs = finish(plan, sketch, gathered)
    return basis, coeffs.reshape(plan.shard_lines, parts, PROBES, nodes)


def solution(mesh):
    param, sensor = mesh.shape["param"], mesh.shape["sensor"]
    assert param % QUAD == 0 and param & (param - 1) == 0 and sensor & (sensor - 1) == 0
    placed = (P(None, None, "sensor", "param"), P(None, None, None, "param"))
    return jax.shard_map(
        functools.partial(on_device, param, sensor),
        mesh=mesh,
        in_specs=placed,
        out_specs=(P(None, None, None, "sensor"), P("sensor", None, None, "param")),
        check_vma=False,
    )
```

```python
import functools

import jax
import jax.numpy as jnp
from jax import lax
from jax.experimental import pallas as pl
from jax.experimental.pallas import tpu as pltpu
from jax.sharding import PartitionSpec as P

LANES = 128
STEP = 2 * LANES
QUAD = 4
PROBES = 4
SPLITS = 3


MIB = 1 << 20


def in_vmem(shape, dtype):
    return pltpu.VMEM(shape, dtype)


def from_vmem(*arrays):
    return [pltpu.with_memory_space_constraint(x, pltpu.VMEM) for x in arrays]


def params(limit):
    return pltpu.CompilerParams(vmem_limit_bytes=limit * MIB)


def roll(x, shift, axis):
    return pltpu.roll(x, shift % x.shape[axis], axis)


def row_of(shape=(8, LANES)):
    return lax.broadcasted_iota(jnp.int32, shape, 0)


def lane_of(shape=(8, LANES)):
    return lax.broadcasted_iota(jnp.int32, shape, 1)


class Plan:
    def __init__(self, lines, parts, group, nodes, shards):
        self.lines, self.parts, self.group, self.nodes = lines, parts, group, nodes
        self.per_line = parts * group
        self.rows = lines * self.per_line
        self.steps = self.rows // STEP
        self.quarter = -(-self.steps // QUAD)
        self.shards = shards
        self.shard_lines = lines // shards
        self.total = parts * lines * group * shards
        assert parts == 2 and nodes == LANES and self.rows % STEP == 0 and self.per_line >= STEP
        assert lines % shards == 0 and self.steps > (QUAD - 1) * self.quarter


def first_line(plan, step):
    return (step * STEP) // plan.per_line


def sketch_kernel(plan, blocks_ref, probes_ref, *rest):
    outs, kept_ref, held_ref, lhs_ref, held_sem, sems = rest[:QUAD], *rest[QUAD:]
    me = lax.axis_index("param") & (QUAD - 1)
    main = plan.quarter - 1
    order = [k for k in range(1, QUAD)] + [0]

    def copies(k):
        first = (me ^ k) * plan.quarter
        tail = jnp.minimum(first + main, plan.steps - 1)
        return (
            pltpu.make_async_copy(
                blocks_ref.at[pl.ds(pl.multiple_of(first * STEP, STEP), main * STEP)],
                kept_ref.at[k, pl.ds(0, main * STEP)],
                sems.at[k, 0],
            ),
            pltpu.make_async_copy(
                blocks_ref.at[pl.ds(pl.multiple_of(tail * STEP, STEP), STEP)],
                kept_ref.at[k, pl.ds(main * STEP, STEP)],
                sems.at[k, 1],
            ),
        )

    load = pltpu.make_async_copy(probes_ref, held_ref, held_sem)
    load.start()
    for k in order:
        for copy in copies(k):
            copy.start()
    load.wait()
    held = plan.lines * 2 * PROBES
    lhs_ref[pl.ds(0, held)] = held_ref[...].astype(jnp.float32)
    lhs_ref[pl.ds(held, 8)] = jnp.zeros((8, LANES), jnp.float32)
    low = row_of() < 4
    even = lane_of() % 2 == 0
    column = lane_of((8, STEP))
    for k in order:
        for copy in copies(k):
            copy.wait()
        first = (me ^ k) * plan.quarter

        def body(t, _, k=k, first=first):
            step = first + t
            line = first_line(plan, jnp.minimum(step, plan.steps - 1))
            probe = lhs_ref[pl.ds(pl.multiple_of(line * 8, 8), 16)].astype(jnp.bfloat16)
            block = kept_ref[k, pl.ds(pl.multiple_of(t * STEP, STEP), STEP)]
            both = lax.dot_general(probe, block, (((1,), (1,)), ((), ())), preferred_element_type=jnp.float32)
            place = column + step * STEP
            own = jnp.where(place < (line + 1) * plan.per_line, both[:8], both[8:])
            own = jnp.where(place < plan.rows, own, 0.0)
            left, right = own[:, :LANES], own[:, LANES:]
            direct = jnp.where(low, left, roll(right, 4, 0))
            crossed = jnp.where(low, roll(left, 4, 0), right)
            outs[k][t] = direct + jnp.where(even, -roll(crossed, -1, 1), roll(crossed, 1, 1))
            return 0

        lax.fori_loop(0, plan.quarter, body, 0, unroll=True)


def sketch_terms(plan, blocks, probes):
    piece = in_vmem((plan.quarter, 8, LANES), jnp.float32)
    kept = in_vmem((QUAD, plan.quarter * STEP, LANES), jnp.bfloat16)
    vmem = pl.BlockSpec(memory_space=pltpu.VMEM)
    return pl.pallas_call(
        functools.partial(sketch_kernel, plan),
        out_shape=[piece] * QUAD + [kept],
        in_specs=[pl.BlockSpec(memory_space=pl.ANY)] * 2,
        out_specs=[vmem] * (QUAD + 1),
        scratch_shapes=[
            pltpu.VMEM((plan.lines * 8, LANES), jnp.bfloat16),
            pltpu.VMEM((plan.lines * 8 + 8, LANES), jnp.float32),
            pltpu.SemaphoreType.DMA(()),
            pltpu.SemaphoreType.DMA((QUAD, 2)),
        ],
        compiler_params=params(16),
        name="sketch_terms",
    )(*[pltpu.with_memory_space_constraint(x, pltpu.HBM) for x in (blocks, probes)])


def gram_kernel(plan, *refs):
    ins, out_ref = refs[:-1], refs[-1]
    row = row_of()
    lane = lane_of()
    sums = [jnp.zeros((8, LANES), jnp.float32) for _ in range(3)]
    for t in range(plan.quarter):
        x = ins[0][t]
        for other in ins[1:]:
            x = x + other[t]
        out_ref[t] = x
        for d in range(3):
            y = x if d == 0 else jnp.where(row % 4 + d < 4, roll(x, -d, 0), roll(x, 4 - d, 0))
            sums[d] = sums[d] + x * y
    packed = jnp.zeros((8, LANES), jnp.float32)
    for d in range(3):
        packed = jnp.where(lane == d, jnp.sum(sums[d], axis=1, keepdims=True), packed)
    out_ref[plan.quarter] = packed


def add_with_gram(plan, *pieces):
    vmem = pl.BlockSpec(memory_space=pltpu.VMEM)
    return pl.pallas_call(
        functools.partial(gram_kernel, plan),
        out_shape=in_vmem((plan.quarter + 1, 8, LANES), jnp.float32),
        in_specs=[vmem] * len(pieces),
        out_specs=vmem,
        compiler_params=params(16),
        name="add_with_gram",
    )(*from_vmem(*pieces))


def adjoint_kernel(plan, kept_ref, *rest):
    ins, outs, acc_ref = rest[:QUAD], rest[QUAD : QUAD + plan.shards], rest[QUAD + plan.shards]
    me = lax.axis_index("param") & (QUAD - 1)
    spot = lax.axis_index("sensor")
    low = row_of() < 4
    even = lane_of() % 2 == 0
    column = lane_of((8, STEP))
    acc_ref[...] = jnp.zeros(acc_ref.shape, jnp.float32)
    for k in range(QUAD):
        first = (me ^ k) * plan.quarter

        def body(t, _, k=k, first=first):
            step = jnp.minimum(first + t, plan.steps - 1)
            line = first_line(plan, step)
            x = ins[k][t]
            y = jnp.where(even, roll(x, -1, 1), -roll(x, 1, 1))
            left = jnp.where(low, x, roll(y, 4, 0))
            right = jnp.where(low, roll(x, 4, 0), y)
            value = jnp.concatenate([left, right], axis=1)
            mine = column + step * STEP < (line + 1) * plan.per_line
            terms = []
            for _ in range(SPLITS):
                term = value.astype(jnp.bfloat16).astype(jnp.float32)
                terms.append(jnp.where(mine, term, 0.0))
                terms.append(jnp.where(mine, 0.0, term))
                value = value - term
            lhs = jnp.concatenate(terms, axis=0).astype(jnp.bfloat16)
            block = kept_ref[k, pl.ds(pl.multiple_of(t * STEP, STEP), STEP)]
            got = jnp.dot(lhs, block, preferred_element_type=jnp.float32)
            here = sum(got[16 * i : 16 * i + 8] for i in range(SPLITS))
            after = sum(got[16 * i + 8 : 16 * i + 16] for i in range(SPLITS))
            acc_ref[line] = acc_ref[line] + here
            acc_ref[line + 1] = acc_ref[line + 1] + after
            return 0

        lax.fori_loop(0, plan.quarter, body, 0, unroll=True)
    packed = sum(ref[plan.quarter] for ref in ins)
    for k in range(plan.shards):
        start = (spot ^ k) * plan.shard_lines
        outs[k][pl.ds(0, plan.shard_lines)] = acc_ref[pl.ds(start, plan.shard_lines)]
        outs[k][plan.shard_lines] = packed


def adjoint_terms(plan, kept, pieces):
    vmem = pl.BlockSpec(memory_space=pltpu.VMEM)
    return pl.pallas_call(
        functools.partial(adjoint_kernel, plan),
        out_shape=[in_vmem((plan.shard_lines + 1, 8, LANES), jnp.float32)] * plan.shards,
        in_specs=[vmem] * (1 + QUAD),
        out_specs=[vmem] * plan.shards,
        scratch_shapes=[pltpu.VMEM((plan.lines + 1, 8, LANES), jnp.float32)],
        compiler_params=params(16),
        name="adjoint_terms",
    )(*from_vmem(kept, *pieces))


def by_line_kernel(plan, *rest):
    ins, out_ref, flat_ref = rest[:QUAD], rest[QUAD], rest[QUAD + 1]
    me = lax.axis_index("param") & (QUAD - 1)
    lane = lane_of()
    half = LANES // 2
    stay = (row_of() < 4) == (lane < half)
    source = jnp.where(lane < half, 2 * lane, 2 * lane - (LANES - 1))
    for k in range(QUAD):
        first = (me ^ k) * plan.quarter
        for t in range(plan.quarter):
            split = jnp.take_along_axis(ins[k][t], source, axis=1)
            flat_ref[first + t] = jnp.where(stay, split, roll(roll(split, 4, 0), half, 1))
    tiles = -(-plan.group // LANES)
    for line in range(plan.lines):
        tile, shift = divmod(line * plan.group, LANES)
        turned = [roll(flat_ref[tile + i], -shift, 1) for i in range(tiles + 1)]
        for i in range(tiles):
            width = min(LANES, plan.group - i * LANES)
            part = jnp.where(lane < LANES - shift, turned[i], turned[i + 1])
            out_ref[line, :, pl.ds(i * LANES, width)] = part[:, :width]


def sketch_by_line(plan, pieces):
    vmem = pl.BlockSpec(memory_space=pltpu.VMEM)
    return pl.pallas_call(
        functools.partial(by_line_kernel, plan),
        out_shape=in_vmem((plan.lines, 8, plan.group), jnp.float32),
        in_specs=[vmem] * QUAD,
        out_specs=vmem,
        scratch_shapes=[pltpu.VMEM((QUAD * plan.quarter + 2, 8, LANES), jnp.float32)],
        compiler_params=params(16),
        name="sketch_by_line",
    )(*from_vmem(*pieces))


def inverse_rows(plan, packed):
    row = row_of()
    lane = lane_of()
    packed = packed + roll(packed, 4, 0)
    entry = {}
    for d in range(3):
        for a in range(PROBES):
            b = (a + d) % PROBES
            if (max(a, b), min(a, b)) not in entry:
                chosen = jnp.where((row == a) & (lane == d), packed, 0.0)
                whole = jnp.sum(jnp.sum(chosen, axis=1, keepdims=True), axis=0, keepdims=True)
                entry[max(a, b), min(a, b)] = jnp.broadcast_to(whole, (8, LANES)) / plan.total
    low = {}
    inv = {}
    for j in range(PROBES):
        rest = entry[j, j]
        for m in range(j):
            rest = rest - low[j, m] * low[j, m]
        low[j, j] = jnp.sqrt(rest)
        inv[j, j] = 1.0 / low[j, j]
        for i in range(j + 1, PROBES):
            rest = entry[i, j]
            for m in range(j):
                rest = rest - low[i, m] * low[j, m]
            low[i, j] = rest * inv[j, j]
    for i in range(PROBES):
        for j in range(i):
            total = sum(low[i, m] * inv[m, j] for m in range(j, i))
            inv[i, j] = -total * inv[i, i]
    rows = []
    for d in range(PROBES):
        value = jnp.zeros((8, LANES), jnp.float32)
        for a in range(d, PROBES):
            value = jnp.where(row % 4 == a, inv[a, a - d], value)
        rows.append(value)
    return rows


def final_kernel(plan, sketch_ref, *rest):
    ins, basis_ref, coeffs_ref = rest[: plan.shards], rest[plan.shards], rest[plan.shards + 1]
    packed = sum(ref[plan.shard_lines] for ref in ins)
    rows = inverse_rows(plan, packed)

    def scaled(x):
        width = x.shape[1]
        return sum((rows[d][:, :width] * (roll(x, d, 0) if d else x)) for d in range(PROBES))

    for pair in range(plan.shard_lines // 2):
        two = [scaled(sum(ref[2 * pair + i] for ref in ins)) for i in range(2)]
        coeffs_ref[pl.ds(16 * pair, 16)] = jnp.concatenate(two, axis=0).astype(jnp.bfloat16)
    for line in range(plan.lines):
        for start in range(0, plan.group, LANES):
            width = min(LANES, plan.group - start)
            value = scaled(sketch_ref[line, :, pl.ds(start, width)])
            for part in range(2):
                basis_ref[line, part, :, pl.ds(start, width)] = value[4 * part : 4 * part + 4]


def finish(plan, sketch, pieces):
    vmem = pl.BlockSpec(memory_space=pltpu.VMEM)
    return pl.pallas_call(
        functools.partial(final_kernel, plan),
        out_shape=[
            jax.ShapeDtypeStruct((plan.lines, 2, PROBES, plan.group), jnp.float32),
            jax.ShapeDtypeStruct((plan.shard_lines * 8, LANES), jnp.bfloat16),
        ],
        in_specs=[vmem] * (1 + plan.shards),
        out_specs=[vmem] * 2,
        compiler_params=params(16),
        name="finish",
    )(*from_vmem(sketch, *pieces))


def trade(x, axis, size, k):
    return lax.ppermute(x, axis, [(i, i ^ k) for i in range(size)])


def on_device(param, sensor, blocks, probes):
    lines, parts, group, nodes = blocks.shape
    plan = Plan(lines, parts, group, nodes, sensor)
    flat_blocks = blocks.transpose(0, 2, 1, 3).reshape(plan.rows, nodes)
    flat_probes = probes.reshape(lines * parts * PROBES, nodes)
    *terms, kept = sketch_terms(plan, flat_blocks, flat_probes)
    total = terms[0] + sum(trade(terms[k], "param", param, k) for k in range(1, QUAD))
    span = QUAD
    while span * 2 < param:
        total = total + trade(total, "param", param, span)
        span *= 2
    sums = [total] + ([trade(total, "param", param, span)] if span < param else [])
    own = add_with_gram(plan, *sums)
    pieces = [own] + [trade(own, "param", param, k) for k in range(1, QUAD)]
    adjoint = adjoint_terms(plan, kept, pieces)
    gathered = [adjoint[0]] + [trade(adjoint[k], "sensor", sensor, k) for k in range(1, sensor)]
    sketch = sketch_by_line(plan, pieces)
    basis, coeffs = finish(plan, sketch, gathered)
    return basis, coeffs.reshape(plan.shard_lines, parts, PROBES, nodes)


def solution(mesh):
    param, sensor = mesh.shape["param"], mesh.shape["sensor"]
    assert param % QUAD == 0 and param & (param - 1) == 0 and sensor & (sensor - 1) == 0
    placed = (P(None, None, "sensor", "param"), P(None, None, None, "param"))
    return jax.shard_map(
        functools.partial(on_device, param, sensor),
        mesh=mesh,
        in_specs=placed,
        out_specs=(P(None, None, None, "sensor"), P("sensor", None, None, "param")),
        check_vma=False,
    )
```

```python
import functools

import jax
import jax.numpy as jnp
from jax import lax
from jax.experimental import pallas as pl
from jax.experimental.pallas import tpu as pltpu
from jax.sharding import PartitionSpec as P

LANES = 128
STEP = 2 * LANES
QUAD = 4
PROBES = 4
ARRIVALS = ((3, 2), (1, 0))
URGENCY = (0, 1)
SPLITS = 3


MIB = 1 << 20


def in_vmem(shape, dtype):
    return pltpu.VMEM(shape, dtype)


def from_vmem(*arrays):
    return [pltpu.with_memory_space_constraint(x, pltpu.VMEM) for x in arrays]


def params(limit):
    return pltpu.CompilerParams(vmem_limit_bytes=limit * MIB)


def roll(x, shift, axis):
    return pltpu.roll(x, shift % x.shape[axis], axis)


def row_of(shape=(8, LANES)):
    return lax.broadcasted_iota(jnp.int32, shape, 0)


def lane_of(shape=(8, LANES)):
    return lax.broadcasted_iota(jnp.int32, shape, 1)


class Plan:
    def __init__(self, lines, parts, group, nodes, shards):
        self.lines, self.parts, self.group, self.nodes = lines, parts, group, nodes
        self.per_line = parts * group
        self.rows = lines * self.per_line
        self.steps = self.rows // STEP
        self.quarter = -(-self.steps // QUAD)
        self.shards = shards
        self.shard_lines = lines // shards
        self.total = parts * lines * group * shards
        assert parts == 2 and nodes == LANES and self.rows % STEP == 0 and self.per_line >= STEP
        assert lines % shards == 0 and self.steps > (QUAD - 1) * self.quarter


def first_line(plan, step):
    return (step * STEP) // plan.per_line


def sketch_kernel(plan, blocks_ref, probes_ref, *rest):
    outs, kept_ref, held_ref, lhs_ref, held_sem, sems = rest[:QUAD], *rest[QUAD:]
    me = lax.axis_index("param") & (QUAD - 1)
    whole = plan.quarter - 1

    def copies(k):
        first = (me ^ k) * plan.quarter
        found = []
        for at, (start, count) in enumerate(((0, whole), (whole, 1))):
            source = jnp.minimum(first + start, plan.steps - count)
            found.append(
                pltpu.make_async_copy(
                    blocks_ref.at[pl.ds(pl.multiple_of(source * STEP, STEP), count * STEP)],
                    kept_ref.at[k, pl.ds(start * STEP, count * STEP)],
                    sems.at[k, at],
                )
            )
        return found

    load = pltpu.make_async_copy(probes_ref, held_ref, held_sem)
    load.start()
    for order, group in enumerate(ARRIVALS):
        for k in group:
            for copy in copies(k):
                copy.start(priority=URGENCY[order])
    load.wait()
    held = plan.lines * 2 * PROBES
    lhs_ref[pl.ds(0, held)] = held_ref[...].astype(jnp.float32)
    lhs_ref[pl.ds(held, 8)] = jnp.zeros((8, LANES), jnp.float32)
    low_rows = row_of() < 4
    even = lane_of() % 2 == 0
    column = lane_of((8, STEP))
    for group in ARRIVALS:
        for k in group:
            for copy in copies(k):
                copy.wait()
        for k in group:
            first = (me ^ k) * plan.quarter

            def body(t, _, k=k, first=first):
                step = first + t
                line = first_line(plan, jnp.minimum(step, plan.steps - 1))
                probe = lhs_ref[pl.ds(pl.multiple_of(line * 8, 8), 16)].astype(jnp.bfloat16)
                block = kept_ref[k, pl.ds(pl.multiple_of(t * STEP, STEP), STEP)]
                both = lax.dot_general(probe, block, (((1,), (1,)), ((), ())), preferred_element_type=jnp.float32)
                place = column + step * STEP
                own = jnp.where(place < (line + 1) * plan.per_line, both[:8], both[8:])
                own = jnp.where(place < plan.rows, own, 0.0)
                left, right = own[:, :LANES], own[:, LANES:]
                direct = jnp.where(low_rows, left, roll(right, 4, 0))
                crossed = jnp.where(low_rows, roll(left, 4, 0), right)
                outs[k][t] = direct + jnp.where(even, -roll(crossed, -1, 1), roll(crossed, 1, 1))
                return 0

            lax.fori_loop(0, plan.quarter, body, 0, unroll=True)


def sketch_terms(plan, blocks, probes):
    piece = in_vmem((plan.quarter, 8, LANES), jnp.float32)
    kept = in_vmem((QUAD, plan.quarter * STEP, LANES), jnp.bfloat16)
    vmem = pl.BlockSpec(memory_space=pltpu.VMEM)
    return pl.pallas_call(
        functools.partial(sketch_kernel, plan),
        out_shape=[piece] * QUAD + [kept],
        in_specs=[pl.BlockSpec(memory_space=pl.ANY)] * 2,
        out_specs=[vmem] * (QUAD + 1),
        scratch_shapes=[
            pltpu.VMEM((plan.lines * 8, LANES), jnp.bfloat16),
            pltpu.VMEM((plan.lines * 8 + 8, LANES), jnp.float32),
            pltpu.SemaphoreType.DMA(()),
            pltpu.SemaphoreType.DMA((QUAD, 2)),
        ],
        compiler_params=params(16),
        name="sketch_terms",
    )(*[pltpu.with_memory_space_constraint(x, pltpu.HBM) for x in (blocks, probes)])


def gram_kernel(plan, *refs):
    ins, out_ref = refs[:-1], refs[-1]
    row = row_of()
    lane = lane_of()
    sums = [jnp.zeros((8, LANES), jnp.float32) for _ in range(3)]
    for t in range(plan.quarter):
        x = ins[0][t]
        for other in ins[1:]:
            x = x + other[t]
        out_ref[t] = x
        for d in range(3):
            y = x if d == 0 else jnp.where(row % 4 + d < 4, roll(x, -d, 0), roll(x, 4 - d, 0))
            sums[d] = sums[d] + x * y
    packed = jnp.zeros((8, LANES), jnp.float32)
    for d in range(3):
        packed = jnp.where(lane == d, jnp.sum(sums[d], axis=1, keepdims=True), packed)
    out_ref[plan.quarter] = packed


def add_with_gram(plan, *pieces):
    vmem = pl.BlockSpec(memory_space=pltpu.VMEM)
    return pl.pallas_call(
        functools.partial(gram_kernel, plan),
        out_shape=in_vmem((plan.quarter + 1, 8, LANES), jnp.float32),
        in_specs=[vmem] * len(pieces),
        out_specs=vmem,
        compiler_params=params(16),
        name="add_with_gram",
    )(*from_vmem(*pieces))


def adjoint_kernel(plan, kept_ref, *rest):
    ins, outs, acc_ref = rest[:QUAD], rest[QUAD : QUAD + plan.shards], rest[QUAD + plan.shards]
    me = lax.axis_index("param") & (QUAD - 1)
    spot = lax.axis_index("sensor")
    low = row_of() < 4
    even = lane_of() % 2 == 0
    column = lane_of((8, STEP))
    acc_ref[...] = jnp.zeros(acc_ref.shape, jnp.float32)
    for k in range(QUAD):
        first = (me ^ k) * plan.quarter

        def body(t, _, k=k, first=first):
            step = jnp.minimum(first + t, plan.steps - 1)
            line = first_line(plan, step)
            x = ins[k][t]
            y = jnp.where(even, roll(x, -1, 1), -roll(x, 1, 1))
            left = jnp.where(low, x, roll(y, 4, 0))
            right = jnp.where(low, roll(x, 4, 0), y)
            value = jnp.concatenate([left, right], axis=1)
            mine = column + step * STEP < (line + 1) * plan.per_line
            terms = []
            for _ in range(SPLITS):
                term = value.astype(jnp.bfloat16).astype(jnp.float32)
                terms.append(jnp.where(mine, term, 0.0))
                terms.append(jnp.where(mine, 0.0, term))
                value = value - term
            lhs = jnp.concatenate(terms, axis=0).astype(jnp.bfloat16)
            block = kept_ref[k, pl.ds(pl.multiple_of(t * STEP, STEP), STEP)]
            got = jnp.dot(lhs, block, preferred_element_type=jnp.float32)
            here = sum(got[16 * i : 16 * i + 8] for i in range(SPLITS))
            after = sum(got[16 * i + 8 : 16 * i + 16] for i in range(SPLITS))
            acc_ref[line] = acc_ref[line] + here
            acc_ref[line + 1] = acc_ref[line + 1] + after
            return 0

        lax.fori_loop(0, plan.quarter, body, 0, unroll=True)
    packed = sum(ref[plan.quarter] for ref in ins)
    for k in range(plan.shards):
        start = (spot ^ k) * plan.shard_lines
        outs[k][pl.ds(0, plan.shard_lines)] = acc_ref[pl.ds(start, plan.shard_lines)]
        outs[k][plan.shard_lines] = packed


def adjoint_terms(plan, kept, pieces):
    vmem = pl.BlockSpec(memory_space=pltpu.VMEM)
    return pl.pallas_call(
        functools.partial(adjoint_kernel, plan),
        out_shape=[in_vmem((plan.shard_lines + 1, 8, LANES), jnp.float32)] * plan.shards,
        in_specs=[vmem] * (1 + QUAD),
        out_specs=[vmem] * plan.shards,
        scratch_shapes=[pltpu.VMEM((plan.lines + 1, 8, LANES), jnp.float32)],
        compiler_params=params(16),
        name="adjoint_terms",
    )(*from_vmem(kept, *pieces))


def by_line_kernel(plan, *rest):
    ins, out_ref, flat_ref = rest[:QUAD], rest[QUAD], rest[QUAD + 1]
    me = lax.axis_index("param") & (QUAD - 1)
    lane = lane_of()
    half = LANES // 2
    stay = (row_of() < 4) == (lane < half)
    source = jnp.where(lane < half, 2 * lane, 2 * lane - (LANES - 1))
    for k in range(QUAD):
        first = (me ^ k) * plan.quarter
        for t in range(plan.quarter):
            split = jnp.take_along_axis(ins[k][t], source, axis=1)
            flat_ref[first + t] = jnp.where(stay, split, roll(roll(split, 4, 0), half, 1))
    tiles = -(-plan.group // LANES)
    for line in range(plan.lines):
        tile, shift = divmod(line * plan.group, LANES)
        turned = [roll(flat_ref[tile + i], -shift, 1) for i in range(tiles + 1)]
        for i in range(tiles):
            width = min(LANES, plan.group - i * LANES)
            part = jnp.where(lane < LANES - shift, turned[i], turned[i + 1])
            out_ref[line, :, pl.ds(i * LANES, width)] = part[:, :width]


def sketch_by_line(plan, pieces):
    vmem = pl.BlockSpec(memory_space=pltpu.VMEM)
    return pl.pallas_call(
        functools.partial(by_line_kernel, plan),
        out_shape=in_vmem((plan.lines, 8, plan.group), jnp.float32),
        in_specs=[vmem] * QUAD,
        out_specs=vmem,
        scratch_shapes=[pltpu.VMEM((QUAD * plan.quarter + 2, 8, LANES), jnp.float32)],
        compiler_params=params(16),
        name="sketch_by_line",
    )(*from_vmem(*pieces))


def inverse_rows(plan, packed):
    row = row_of()
    lane = lane_of()
    packed = packed + roll(packed, 4, 0)
    entry = {}
    for d in range(3):
        for a in range(PROBES):
            b = (a + d) % PROBES
            if (max(a, b), min(a, b)) not in entry:
                chosen = jnp.where((row == a) & (lane == d), packed, 0.0)
                whole = jnp.sum(jnp.sum(chosen, axis=1, keepdims=True), axis=0, keepdims=True)
                entry[max(a, b), min(a, b)] = jnp.broadcast_to(whole, (8, LANES)) / plan.total
    low = {}
    inv = {}
    for j in range(PROBES):
        rest = entry[j, j]
        for m in range(j):
            rest = rest - low[j, m] * low[j, m]
        low[j, j] = jnp.sqrt(rest)
        inv[j, j] = 1.0 / low[j, j]
        for i in range(j + 1, PROBES):
            rest = entry[i, j]
            for m in range(j):
                rest = rest - low[i, m] * low[j, m]
            low[i, j] = rest * inv[j, j]
    for i in range(PROBES):
        for j in range(i):
            total = sum(low[i, m] * inv[m, j] for m in range(j, i))
            inv[i, j] = -total * inv[i, i]
    rows = []
    for d in range(PROBES):
        value = jnp.zeros((8, LANES), jnp.float32)
        for a in range(d, PROBES):
            value = jnp.where(row % 4 == a, inv[a, a - d], value)
        rows.append(value)
    return rows


def final_kernel(plan, sketch_ref, *rest):
    ins, basis_ref, coeffs_ref = rest[: plan.shards], rest[plan.shards], rest[plan.shards + 1]
    packed = sum(ref[plan.shard_lines] for ref in ins)
    rows = inverse_rows(plan, packed)

    def scaled(x):
        width = x.shape[1]
        return sum((rows[d][:, :width] * (roll(x, d, 0) if d else x)) for d in range(PROBES))

    for pair in range(plan.shard_lines // 2):
        two = [scaled(sum(ref[2 * pair + i] for ref in ins)) for i in range(2)]
        coeffs_ref[pl.ds(16 * pair, 16)] = jnp.concatenate(two, axis=0).astype(jnp.bfloat16)
    for line in range(plan.lines):
        for start in range(0, plan.group, LANES):
            width = min(LANES, plan.group - start)
            value = scaled(sketch_ref[line, :, pl.ds(start, width)])
            for part in range(2):
                basis_ref[line, part, :, pl.ds(start, width)] = value[4 * part : 4 * part + 4]


def finish(plan, sketch, pieces):
    vmem = pl.BlockSpec(memory_space=pltpu.VMEM)
    return pl.pallas_call(
        functools.partial(final_kernel, plan),
        out_shape=[
            jax.ShapeDtypeStruct((plan.lines, 2, PROBES, plan.group), jnp.float32),
            jax.ShapeDtypeStruct((plan.shard_lines * 8, LANES), jnp.bfloat16),
        ],
        in_specs=[vmem] * (1 + plan.shards),
        out_specs=[vmem] * 2,
        compiler_params=params(16),
        name="finish",
    )(*from_vmem(sketch, *pieces))


def trade(x, axis, size, k):
    return lax.ppermute(x, axis, [(i, i ^ k) for i in range(size)])


def on_device(param, sensor, blocks, probes):
    lines, parts, group, nodes = blocks.shape
    plan = Plan(lines, parts, group, nodes, sensor)
    flat_blocks = blocks.transpose(0, 2, 1, 3).reshape(plan.rows, nodes)
    flat_probes = probes.reshape(lines * parts * PROBES, nodes)
    *terms, kept = sketch_terms(plan, flat_blocks, flat_probes)
    total = terms[0] + sum(trade(terms[k], "param", param, k) for k in reversed(range(1, QUAD)))
    span = QUAD
    while span * 2 < param:
        total = total + trade(total, "param", param, span)
        span *= 2
    sums = [total] + ([trade(total, "param", param, span)] if span < param else [])
    own = add_with_gram(plan, *sums)
    pieces = [own] + [trade(own, "param", param, k) for k in range(1, QUAD)]
    adjoint = adjoint_terms(plan, kept, pieces)
    gathered = [adjoint[0]] + [trade(adjoint[k], "sensor", sensor, k) for k in range(1, sensor)]
    sketch = sketch_by_line(plan, pieces)
    basis, coeffs = finish(plan, sketch, gathered)
    return basis, coeffs.reshape(plan.shard_lines, parts, PROBES, nodes)


def solution(mesh):
    param, sensor = mesh.shape["param"], mesh.shape["sensor"]
    assert param % QUAD == 0 and param & (param - 1) == 0 and sensor & (sensor - 1) == 0
    placed = (P(None, None, "sensor", "param"), P(None, None, None, "param"))
    return jax.shard_map(
        functools.partial(on_device, param, sensor),
        mesh=mesh,
        in_specs=placed,
        out_specs=(P(None, None, None, "sensor"), P("sensor", None, None, "param")),
        check_vma=False,
    )
```

```python
import functools

import jax
import jax.numpy as jnp
from jax import lax
from jax.experimental import pallas as pl
from jax.experimental.pallas import tpu as pltpu
from jax.sharding import PartitionSpec as P


LANES = 128
STEP = 2 * LANES
QUAD = 4
PROBES = 4
FAR, NEAR = 3, (2, 1, 0)
SPLITS = 3


MIB = 1 << 20


def in_vmem(shape, dtype):
    return pltpu.VMEM(shape, dtype)


def from_vmem(*arrays):
    return [pltpu.with_memory_space_constraint(x, pltpu.VMEM) for x in arrays]


def params(limit):
    return pltpu.CompilerParams(vmem_limit_bytes=limit * MIB)


def roll(x, shift, axis):
    return pltpu.roll(x, shift % x.shape[axis], axis)


def row_of(shape=(8, LANES)):
    return lax.broadcasted_iota(jnp.int32, shape, 0)


def lane_of(shape=(8, LANES)):
    return lax.broadcasted_iota(jnp.int32, shape, 1)


class Plan:
    def __init__(self, lines, parts, group, nodes, shards):
        self.lines, self.parts, self.group, self.nodes = lines, parts, group, nodes
        self.per_line = parts * group
        self.rows = lines * self.per_line
        self.steps = self.rows // STEP
        self.quarter = -(-self.steps // QUAD)
        self.shards = shards
        self.shard_lines = lines // shards
        self.total = parts * lines * group * shards
        assert parts == 2 and nodes == LANES and self.rows % STEP == 0 and self.per_line >= STEP
        assert lines % shards == 0 and self.steps > (QUAD - 1) * self.quarter


def first_line(plan, step):
    return (step * STEP) // plan.per_line


def sketch_steps(plan, k, block_at, lhs_ref, out_ref):
    first = (lax.axis_index("param") & (QUAD - 1) ^ k) * plan.quarter
    low = row_of() < 4
    even = lane_of() % 2 == 0
    column = lane_of((8, STEP))

    def body(t, _):
        step = first + t
        used = jnp.minimum(step, plan.steps - 1)
        line = first_line(plan, used)
        probe = lhs_ref[pl.ds(pl.multiple_of(line * 8, 8), 16)].astype(jnp.bfloat16)
        both = lax.dot_general(
            probe, block_at(t, used), (((1,), (1,)), ((), ())), preferred_element_type=jnp.float32
        )
        place = column + step * STEP
        own = jnp.where(place < (line + 1) * plan.per_line, both[:8], both[8:])
        own = jnp.where(place < plan.rows, own, 0.0)
        left, right = own[:, :LANES], own[:, LANES:]
        direct = jnp.where(low, left, roll(right, 4, 0))
        crossed = jnp.where(low, roll(left, 4, 0), right)
        out_ref[t] = direct + jnp.where(even, -roll(crossed, -1, 1), roll(crossed, 1, 1))
        return 0

    lax.fori_loop(0, plan.quarter, body, 0, unroll=True)


def spread_probes(plan, probes_ref, lhs_ref):
    held = plan.lines * 2 * PROBES
    lhs_ref[pl.ds(0, held)] = probes_ref[...].astype(jnp.float32)
    lhs_ref[pl.ds(held, 8)] = jnp.zeros((8, LANES), jnp.float32)


def far_kernel(plan, blocks_ref, probes_ref, out_ref, lhs_ref, held_ref, here_ref, sems):
    first = (lax.axis_index("param") & (QUAD - 1) ^ FAR) * plan.quarter
    whole = plan.quarter - 1
    copies = []
    for at, (start, count) in enumerate(((0, whole), (whole, 1))):
        source = jnp.minimum(first + start, plan.steps - count)
        copies.append(
            pltpu.make_async_copy(
                blocks_ref.at[pl.ds(pl.multiple_of(source * STEP, STEP), count * STEP)],
                here_ref.at[pl.ds(start * STEP, count * STEP)],
                sems.at[at],
            )
        )
    copies.append(pltpu.make_async_copy(probes_ref, held_ref, sems.at[2]))
    for copy in copies:
        copy.start()
    copies[2].wait()
    spread_probes(plan, held_ref, lhs_ref)
    copies[0].wait()
    copies[1].wait()

    def block_at(t, used):
        return here_ref[pl.ds(pl.multiple_of(t * STEP, STEP), STEP)]

    sketch_steps(plan, FAR, block_at, lhs_ref, out_ref)


def near_kernel(plan, blocks_ref, lhs_ref, *outs):
    def block_at(t, used):
        return blocks_ref[pl.ds(pl.multiple_of(used * STEP, STEP), STEP)]

    for k, out_ref in zip(NEAR, outs):
        sketch_steps(plan, k, block_at, lhs_ref, out_ref)


def far_terms(plan, blocks, probes):
    piece = in_vmem((plan.quarter, 8, LANES), jnp.float32)
    lhs = in_vmem((plan.lines * 8 + 8, LANES), jnp.float32)
    vmem = pl.BlockSpec(memory_space=pltpu.VMEM)
    return pl.pallas_call(
        functools.partial(far_kernel, plan),
        out_shape=[piece, lhs],
        in_specs=[pl.BlockSpec(memory_space=pl.ANY)] * 2,
        out_specs=[vmem] * 2,
        scratch_shapes=[
            pltpu.VMEM((plan.lines * 8, LANES), jnp.bfloat16),
            pltpu.VMEM((plan.quarter * STEP, LANES), jnp.bfloat16),
            pltpu.SemaphoreType.DMA((3,)),
        ],
        compiler_params=params(16),
        name="far_terms",
    )(*[pltpu.with_memory_space_constraint(x, pltpu.HBM) for x in (blocks, probes)])


def near_terms(plan, blocks, lhs):
    piece = in_vmem((plan.quarter, 8, LANES), jnp.float32)
    vmem = pl.BlockSpec(memory_space=pltpu.VMEM)
    return pl.pallas_call(
        functools.partial(near_kernel, plan),
        out_shape=[piece] * len(NEAR),
        in_specs=[vmem] * 2,
        out_specs=[vmem] * len(NEAR),
        compiler_params=params(16),
        name="near_terms",
    )(*from_vmem(blocks, lhs))


def gram_kernel(plan, *refs):
    ins, out_ref = refs[:-1], refs[-1]
    row = row_of()
    lane = lane_of()
    sums = [jnp.zeros((8, LANES), jnp.float32) for _ in range(3)]
    for t in range(plan.quarter):
        x = ins[0][t]
        for other in ins[1:]:
            x = x + other[t]
        out_ref[t] = x
        for d in range(3):
            y = x if d == 0 else jnp.where(row % 4 + d < 4, roll(x, -d, 0), roll(x, 4 - d, 0))
            sums[d] = sums[d] + x * y
    packed = jnp.zeros((8, LANES), jnp.float32)
    for d in range(3):
        packed = jnp.where(lane == d, jnp.sum(sums[d], axis=1, keepdims=True), packed)
    out_ref[plan.quarter] = packed


def add_with_gram(plan, *pieces):
    vmem = pl.BlockSpec(memory_space=pltpu.VMEM)
    return pl.pallas_call(
        functools.partial(gram_kernel, plan),
        out_shape=in_vmem((plan.quarter + 1, 8, LANES), jnp.float32),
        in_specs=[vmem] * len(pieces),
        out_specs=vmem,
        compiler_params=params(16),
        name="add_with_gram",
    )(*from_vmem(*pieces))


def adjoint_kernel(plan, blocks_ref, *rest):
    ins, outs, acc_ref = rest[:QUAD], rest[QUAD : QUAD + plan.shards], rest[QUAD + plan.shards]
    me = lax.axis_index("param") & (QUAD - 1)
    spot = lax.axis_index("sensor")
    low = row_of() < 4
    even = lane_of() % 2 == 0
    column = lane_of((8, STEP))
    acc_ref[...] = jnp.zeros(acc_ref.shape, jnp.float32)
    for k in range(QUAD):
        first = (me ^ k) * plan.quarter

        def body(t, _, k=k, first=first):
            step = jnp.minimum(first + t, plan.steps - 1)
            line = first_line(plan, step)
            x = ins[k][t]
            y = jnp.where(even, roll(x, -1, 1), -roll(x, 1, 1))
            left = jnp.where(low, x, roll(y, 4, 0))
            right = jnp.where(low, roll(x, 4, 0), y)
            value = jnp.concatenate([left, right], axis=1)
            mine = column + step * STEP < (line + 1) * plan.per_line
            terms = []
            for _ in range(SPLITS):
                term = value.astype(jnp.bfloat16).astype(jnp.float32)
                terms.append(jnp.where(mine, term, 0.0))
                terms.append(jnp.where(mine, 0.0, term))
                value = value - term
            lhs = jnp.concatenate(terms, axis=0).astype(jnp.bfloat16)
            block = blocks_ref[pl.ds(pl.multiple_of(step * STEP, STEP), STEP)]
            got = jnp.dot(lhs, block, preferred_element_type=jnp.float32)
            here = sum(got[16 * i : 16 * i + 8] for i in range(SPLITS))
            after = sum(got[16 * i + 8 : 16 * i + 16] for i in range(SPLITS))
            acc_ref[line] = acc_ref[line] + here
            acc_ref[line + 1] = acc_ref[line + 1] + after
            return 0

        lax.fori_loop(0, plan.quarter, body, 0, unroll=True)
    packed = sum(ref[plan.quarter] for ref in ins)
    for k in range(plan.shards):
        start = (spot ^ k) * plan.shard_lines
        outs[k][pl.ds(0, plan.shard_lines)] = acc_ref[pl.ds(start, plan.shard_lines)]
        outs[k][plan.shard_lines] = packed


def adjoint_terms(plan, blocks, pieces):
    vmem = pl.BlockSpec(memory_space=pltpu.VMEM)
    return pl.pallas_call(
        functools.partial(adjoint_kernel, plan),
        out_shape=[in_vmem((plan.shard_lines + 1, 8, LANES), jnp.float32)] * plan.shards,
        in_specs=[vmem] * (1 + QUAD),
        out_specs=[vmem] * plan.shards,
        scratch_shapes=[pltpu.VMEM((plan.lines + 1, 8, LANES), jnp.float32)],
        compiler_params=params(16),
        name="adjoint_terms",
    )(*from_vmem(blocks, *pieces))


def by_line_kernel(plan, *rest):
    ins, out_ref, flat_ref = rest[:QUAD], rest[QUAD], rest[QUAD + 1]
    me = lax.axis_index("param") & (QUAD - 1)
    lane = lane_of()
    half = LANES // 2
    stay = (row_of() < 4) == (lane < half)
    source = jnp.where(lane < half, 2 * lane, 2 * lane - (LANES - 1))
    for k in range(QUAD):
        first = (me ^ k) * plan.quarter
        for t in range(plan.quarter):
            split = jnp.take_along_axis(ins[k][t], source, axis=1)
            flat_ref[first + t] = jnp.where(stay, split, roll(roll(split, 4, 0), half, 1))
    tiles = -(-plan.group // LANES)
    for line in range(plan.lines):
        tile, shift = divmod(line * plan.group, LANES)
        turned = [roll(flat_ref[tile + i], -shift, 1) for i in range(tiles + 1)]
        for i in range(tiles):
            width = min(LANES, plan.group - i * LANES)
            part = jnp.where(lane < LANES - shift, turned[i], turned[i + 1])
            out_ref[line, :, pl.ds(i * LANES, width)] = part[:, :width]


def sketch_by_line(plan, pieces):
    vmem = pl.BlockSpec(memory_space=pltpu.VMEM)
    return pl.pallas_call(
        functools.partial(by_line_kernel, plan),
        out_shape=in_vmem((plan.lines, 8, plan.group), jnp.float32),
        in_specs=[vmem] * QUAD,
        out_specs=vmem,
        scratch_shapes=[pltpu.VMEM((QUAD * plan.quarter + 2, 8, LANES), jnp.float32)],
        compiler_params=params(16),
        name="sketch_by_line",
    )(*from_vmem(*pieces))


def inverse_rows(plan, packed):
    row = row_of()
    lane = lane_of()
    packed = packed + roll(packed, 4, 0)
    entry = {}
    for d in range(3):
        for a in range(PROBES):
            b = (a + d) % PROBES
            if (max(a, b), min(a, b)) not in entry:
                chosen = jnp.where((row == a) & (lane == d), packed, 0.0)
                whole = jnp.sum(jnp.sum(chosen, axis=1, keepdims=True), axis=0, keepdims=True)
                entry[max(a, b), min(a, b)] = jnp.broadcast_to(whole, (8, LANES)) / plan.total
    low = {}
    inv = {}
    for j in range(PROBES):
        rest = entry[j, j]
        for m in range(j):
            rest = rest - low[j, m] * low[j, m]
        low[j, j] = jnp.sqrt(rest)
        inv[j, j] = 1.0 / low[j, j]
        for i in range(j + 1, PROBES):
            rest = entry[i, j]
            for m in range(j):
                rest = rest - low[i, m] * low[j, m]
            low[i, j] = rest * inv[j, j]
    for i in range(PROBES):
        for j in range(i):
            total = sum(low[i, m] * inv[m, j] for m in range(j, i))
            inv[i, j] = -total * inv[i, i]
    rows = []
    for d in range(PROBES):
        value = jnp.zeros((8, LANES), jnp.float32)
        for a in range(d, PROBES):
            value = jnp.where(row % 4 == a, inv[a, a - d], value)
        rows.append(value)
    return rows


def final_kernel(plan, sketch_ref, *rest):
    ins, basis_ref, coeffs_ref = rest[: plan.shards], rest[plan.shards], rest[plan.shards + 1]
    packed = sum(ref[plan.shard_lines] for ref in ins)
    rows = inverse_rows(plan, packed)

    def scaled(x):
        width = x.shape[1]
        return sum((rows[d][:, :width] * (roll(x, d, 0) if d else x)) for d in range(PROBES))

    for pair in range(plan.shard_lines // 2):
        two = [scaled(sum(ref[2 * pair + i] for ref in ins)) for i in range(2)]
        coeffs_ref[pl.ds(16 * pair, 16)] = jnp.concatenate(two, axis=0).astype(jnp.bfloat16)
    for line in range(plan.lines):
        for start in range(0, plan.group, LANES):
            width = min(LANES, plan.group - start)
            value = scaled(sketch_ref[line, :, pl.ds(start, width)])
            for part in range(2):
                basis_ref[line, part, :, pl.ds(start, width)] = value[4 * part : 4 * part + 4]


def finish(plan, sketch, pieces):
    vmem = pl.BlockSpec(memory_space=pltpu.VMEM)
    return pl.pallas_call(
        functools.partial(final_kernel, plan),
        out_shape=[
            jax.ShapeDtypeStruct((plan.lines, 2, PROBES, plan.group), jnp.float32),
            jax.ShapeDtypeStruct((plan.shard_lines * 8, LANES), jnp.bfloat16),
        ],
        in_specs=[vmem] * (1 + plan.shards),
        out_specs=[vmem] * 2,
        compiler_params=params(16),
        name="finish",
    )(*from_vmem(sketch, *pieces))


def trade(x, axis, size, k):
    return lax.ppermute(x, axis, [(i, i ^ k) for i in range(size)])


def on_device(param, sensor, blocks, probes):
    return sketch_and_adjoint(param, sensor, blocks, probes)


def sketch_and_adjoint(param, sensor, blocks, probes):
    lines, parts, group, nodes = blocks.shape
    plan = Plan(lines, parts, group, nodes, sensor)
    flat_blocks = blocks.transpose(0, 2, 1, 3).reshape(plan.rows, nodes)
    flat_probes = probes.reshape(lines * parts * PROBES, nodes)
    far, lhs = far_terms(plan, flat_blocks, flat_probes)
    far = trade(far, "param", param, FAR)
    near = near_terms(plan, flat_blocks, lhs)
    total = near[-1] + far
    for k, piece in zip(NEAR[:-1], near):
        total = total + trade(piece, "param", param, k)
    span = QUAD
    while span * 2 < param:
        total = total + trade(total, "param", param, span)
        span *= 2
    sums = [total] + ([trade(total, "param", param, span)] if span < param else [])
    own = add_with_gram(plan, *sums)
    pieces = [own] + [trade(own, "param", param, k) for k in range(1, QUAD)]
    adjoint = adjoint_terms(plan, flat_blocks, pieces)
    gathered = [adjoint[0]] + [trade(adjoint[k], "sensor", sensor, k) for k in range(1, sensor)]
    sketch = sketch_by_line(plan, pieces)
    basis, coeffs = finish(plan, sketch, gathered)
    return basis, coeffs.reshape(plan.shard_lines, parts, PROBES, nodes)


def solution(mesh):
    param, sensor = mesh.shape["param"], mesh.shape["sensor"]
    assert param % QUAD == 0 and param & (param - 1) == 0 and sensor & (sensor - 1) == 0
    placed = (P(None, None, "sensor", "param"), P(None, None, None, "param"))
    return jax.shard_map(
        functools.partial(on_device, param, sensor),
        mesh=mesh,
        in_specs=placed,
        out_specs=(P(None, None, None, "sensor"), P("sensor", None, None, "param")),
        check_vma=False,
    )
```

```python
import functools

import jax
import jax.numpy as jnp
from jax import lax
from jax.experimental import pallas as pl
from jax.experimental.pallas import tpu as pltpu
from jax.sharding import PartitionSpec as P


LANES = 128
STEP = 2 * LANES
QUAD = 4
PROBES = 4
ARRIVALS = ((3, 2), (1,))
REDUCE, GATHER = (3, 2, 1), (3, 2, 1)
URGENCY = (0, 1)
SPLITS = 3


MIB = 1 << 20


def in_vmem(shape, dtype):
    return pltpu.VMEM(shape, dtype)


def from_vmem(*arrays):
    return [pltpu.with_memory_space_constraint(x, pltpu.VMEM) for x in arrays]


def params(limit):
    return pltpu.CompilerParams(vmem_limit_bytes=limit * MIB)


def roll(x, shift, axis):
    return pltpu.roll(x, shift % x.shape[axis], axis)


def row_of(shape=(8, LANES)):
    return lax.broadcasted_iota(jnp.int32, shape, 0)


def lane_of(shape=(8, LANES)):
    return lax.broadcasted_iota(jnp.int32, shape, 1)


class Plan:
    def __init__(self, lines, parts, group, nodes, shards):
        self.lines, self.parts, self.group, self.nodes = lines, parts, group, nodes
        self.per_line = parts * group
        self.rows = lines * self.per_line
        self.steps = self.rows // STEP
        self.quarter = -(-self.steps // QUAD)
        self.shards = shards
        self.shard_lines = lines // shards
        self.total = parts * lines * group * shards
        assert parts == 2 and nodes == LANES and self.rows % STEP == 0 and self.per_line >= STEP
        assert lines % shards == 0 and self.steps > (QUAD - 1) * self.quarter


def first_line(plan, step):
    return (step * STEP) // plan.per_line


def quarter_copies(plan, k, blocks_ref, kept_ref, sems):
    first = (lax.axis_index("param") & (QUAD - 1) ^ k) * plan.quarter
    whole = plan.quarter - 1
    found = []
    for at, (start, count) in enumerate(((0, whole), (whole, 1))):
        source = jnp.minimum(first + start, plan.steps - count)
        found.append(
            pltpu.make_async_copy(
                blocks_ref.at[pl.ds(pl.multiple_of(source * STEP, STEP), count * STEP)],
                kept_ref.at[pl.ds(start * STEP, count * STEP)],
                sems.at[at],
            )
        )
    return found


def quarter_terms(plan, k, kept_ref, lhs_ref, out_ref):
    first = (lax.axis_index("param") & (QUAD - 1) ^ k) * plan.quarter
    low = row_of() < 4
    even = lane_of() % 2 == 0
    column = lane_of((8, STEP))

    def body(t, _):
        step = first + t
        line = first_line(plan, jnp.minimum(step, plan.steps - 1))
        probe = lhs_ref[pl.ds(pl.multiple_of(line * 8, 8), 16)].astype(jnp.bfloat16)
        block = kept_ref[pl.ds(pl.multiple_of(t * STEP, STEP), STEP)]
        both = lax.dot_general(probe, block, (((1,), (1,)), ((), ())), preferred_element_type=jnp.float32)
        place = column + step * STEP
        own = jnp.where(place < (line + 1) * plan.per_line, both[:8], both[8:])
        own = jnp.where(place < plan.rows, own, 0.0)
        left, right = own[:, :LANES], own[:, LANES:]
        direct = jnp.where(low, left, roll(right, 4, 0))
        crossed = jnp.where(low, roll(left, 4, 0), right)
        out_ref[t] = direct + jnp.where(even, -roll(crossed, -1, 1), roll(crossed, 1, 1))
        return 0

    lax.fori_loop(0, plan.quarter, body, 0, unroll=True)


def sent_kernel(plan, blocks_ref, probes_ref, *rest):
    count = QUAD - 1
    outs, kepts, (lhs_ref, held_ref, held_sem, sems) = rest[:count], rest[count : 2 * count], rest[2 * count :]
    load = pltpu.make_async_copy(probes_ref, held_ref, held_sem)
    load.start()
    copies = {k: quarter_copies(plan, k, blocks_ref, kept_ref, sems.at[k]) for k, kept_ref in zip(REDUCE, kepts)}
    for order, group in enumerate(ARRIVALS):
        for k in group:
            for copy in copies[k]:
                copy.start(priority=URGENCY[order])
    load.wait()
    held = plan.lines * 2 * PROBES
    lhs_ref[pl.ds(0, held)] = held_ref[...].astype(jnp.float32)
    lhs_ref[pl.ds(held, 8)] = jnp.zeros((8, LANES), jnp.float32)
    for group in ARRIVALS:
        for k in group:
            for copy in copies[k]:
                copy.wait()
        for k in group:
            at = REDUCE.index(k)
            quarter_terms(plan, k, kepts[at], lhs_ref, outs[at])


def own_kernel(plan, blocks_ref, lhs_ref, out_ref, kept_ref, sems):
    copies = quarter_copies(plan, 0, blocks_ref, kept_ref, sems)
    for copy in copies:
        copy.start()
    for copy in copies:
        copy.wait()
    quarter_terms(plan, 0, kept_ref, lhs_ref, out_ref)


def sketch_terms(plan, blocks, probes):
    piece = in_vmem((plan.quarter, 8, LANES), jnp.float32)
    kept = in_vmem((plan.quarter * STEP, LANES), jnp.bfloat16)
    lhs = in_vmem((plan.lines * 8 + 8, LANES), jnp.float32)
    vmem = pl.BlockSpec(memory_space=pltpu.VMEM)
    count = QUAD - 1
    out = pl.pallas_call(
        functools.partial(sent_kernel, plan),
        out_shape=[piece] * count + [kept] * count + [lhs],
        in_specs=[pl.BlockSpec(memory_space=pl.ANY)] * 2,
        out_specs=[vmem] * (2 * count + 1),
        scratch_shapes=[
            pltpu.VMEM((plan.lines * 8, LANES), jnp.bfloat16),
            pltpu.SemaphoreType.DMA(()),
            pltpu.SemaphoreType.DMA((QUAD, 2)),
        ],
        compiler_params=params(16),
        name="sent_terms",
    )(*[pltpu.with_memory_space_constraint(x, pltpu.HBM) for x in (blocks, probes)])
    return dict(zip(REDUCE, out[:count])), dict(zip(REDUCE, out[count:-1])), out[-1]


def own_terms(plan, blocks, lhs):
    vmem = pl.BlockSpec(memory_space=pltpu.VMEM)
    return pl.pallas_call(
        functools.partial(own_kernel, plan),
        out_shape=[
            in_vmem((plan.quarter, 8, LANES), jnp.float32),
            in_vmem((plan.quarter * STEP, LANES), jnp.bfloat16),
        ],
        in_specs=[pl.BlockSpec(memory_space=pl.ANY), vmem],
        out_specs=[vmem] * 2,
        scratch_shapes=[pltpu.SemaphoreType.DMA((2,))],
        compiler_params=params(16),
        name="own_terms",
    )(pltpu.with_memory_space_constraint(blocks, pltpu.HBM), *from_vmem(lhs))


def gram_kernel(plan, *refs):
    ins, out_ref = refs[:-1], refs[-1]
    row = row_of()
    lane = lane_of()
    sums = [jnp.zeros((8, LANES), jnp.float32) for _ in range(3)]
    for t in range(plan.quarter):
        x = ins[0][t]
        for other in ins[1:]:
            x = x + other[t]
        out_ref[t] = x
        for d in range(3):
            y = x if d == 0 else jnp.where(row % 4 + d < 4, roll(x, -d, 0), roll(x, 4 - d, 0))
            sums[d] = sums[d] + x * y
    packed = jnp.zeros((8, LANES), jnp.float32)
    for d in range(3):
        packed = jnp.where(lane == d, jnp.sum(sums[d], axis=1, keepdims=True), packed)
    out_ref[plan.quarter] = packed


def add_with_gram(plan, *pieces):
    vmem = pl.BlockSpec(memory_space=pltpu.VMEM)
    return pl.pallas_call(
        functools.partial(gram_kernel, plan),
        out_shape=in_vmem((plan.quarter + 1, 8, LANES), jnp.float32),
        in_specs=[vmem] * len(pieces),
        out_specs=vmem,
        compiler_params=params(16),
        name="add_with_gram",
    )(*from_vmem(*pieces))


def adjoint_kernel(plan, distances, count, *refs):
    ins, kepts, rest = refs[:count], refs[count : 2 * count], refs[2 * count :]
    earlier = rest[0] if len(rest) > 1 else None
    acc_ref = rest[-1]
    param = lax.axis_index("param")
    low = row_of() < 4
    even = lane_of() % 2 == 0
    column = lane_of((8, STEP))
    acc_ref[...] = jnp.zeros(acc_ref.shape, jnp.float32)
    for k, in_ref, kept_ref in zip(distances, ins, kepts):
        first = (param & (QUAD - 1) ^ k) * plan.quarter

        def body(t, _, first=first, in_ref=in_ref, kept_ref=kept_ref):
            step = jnp.minimum(first + t, plan.steps - 1)
            line = first_line(plan, step)
            x = in_ref[t]
            y = jnp.where(even, roll(x, -1, 1), -roll(x, 1, 1))
            left = jnp.where(low, x, roll(y, 4, 0))
            right = jnp.where(low, roll(x, 4, 0), y)
            value = jnp.concatenate([left, right], axis=1)
            mine = column + step * STEP < (line + 1) * plan.per_line
            terms = []
            for _ in range(SPLITS):
                term = value.astype(jnp.bfloat16).astype(jnp.float32)
                terms.append(jnp.where(mine, term, 0.0))
                terms.append(jnp.where(mine, 0.0, term))
                value = value - term
            lhs = jnp.concatenate(terms, axis=0).astype(jnp.bfloat16)
            block = kept_ref[pl.ds(pl.multiple_of(t * STEP, STEP), STEP)]
            got = jnp.dot(lhs, block, preferred_element_type=jnp.float32)
            here = sum(got[16 * i : 16 * i + 8] for i in range(SPLITS))
            after = sum(got[16 * i + 8 : 16 * i + 16] for i in range(SPLITS))
            acc_ref[line] = acc_ref[line] + here
            acc_ref[line + 1] = acc_ref[line + 1] + after
            return 0

        lax.fori_loop(0, plan.quarter, body, 0, unroll=True)
    packed = sum(ref[plan.quarter] for ref in ins)
    if earlier is None:
        acc_ref[plan.lines] = packed
        return
    packed = packed + earlier[plan.lines]
    spot = lax.axis_index("sensor")
    for k, out_ref in enumerate(rest[1:-1]):
        lines = pl.ds((spot ^ k) * plan.shard_lines, plan.shard_lines)
        out_ref[pl.ds(0, plan.shard_lines)] = acc_ref[lines] + earlier[lines]
        out_ref[plan.shard_lines] = packed


def adjoint_terms(plan, distances, pieces, kept, earlier=None):
    vmem = pl.BlockSpec(memory_space=pltpu.VMEM)
    whole = in_vmem((plan.lines + 1, 8, LANES), jnp.float32)
    shard = in_vmem((plan.shard_lines + 1, 8, LANES), jnp.float32)
    given = [pieces[k] for k in distances] + [kept[k] for k in distances]
    if earlier is not None:
        given.append(earlier)
    return pl.pallas_call(
        functools.partial(adjoint_kernel, plan, distances, len(distances)),
        out_shape=whole if earlier is None else [shard] * plan.shards,
        in_specs=[vmem] * len(given),
        out_specs=vmem if earlier is None else [vmem] * plan.shards,
        scratch_shapes=[] if earlier is None else [whole],
        compiler_params=params(16),
        name="adjoint_first" if earlier is None else "adjoint_rest",
    )(*from_vmem(*given))


def by_line_kernel(plan, *rest):
    ins, out_ref, flat_ref = rest[:QUAD], rest[QUAD], rest[QUAD + 1]
    me = lax.axis_index("param") & (QUAD - 1)
    lane = lane_of()
    half = LANES // 2
    stay = (row_of() < 4) == (lane < half)
    source = jnp.where(lane < half, 2 * lane, 2 * lane - (LANES - 1))
    for k in range(QUAD):
        first = (me ^ k) * plan.quarter
        for t in range(plan.quarter):
            split = jnp.take_along_axis(ins[k][t], source, axis=1)
            flat_ref[first + t] = jnp.where(stay, split, roll(roll(split, 4, 0), half, 1))
    tiles = -(-plan.group // LANES)
    for line in range(plan.lines):
        tile, shift = divmod(line * plan.group, LANES)
        turned = [roll(flat_ref[tile + i], -shift, 1) for i in range(tiles + 1)]
        for i in range(tiles):
            width = min(LANES, plan.group - i * LANES)
            part = jnp.where(lane < LANES - shift, turned[i], turned[i + 1])
            out_ref[line, :, pl.ds(i * LANES, width)] = part[:, :width]


def sketch_by_line(plan, pieces):
    vmem = pl.BlockSpec(memory_space=pltpu.VMEM)
    return pl.pallas_call(
        functools.partial(by_line_kernel, plan),
        out_shape=in_vmem((plan.lines, 8, plan.group), jnp.float32),
        in_specs=[vmem] * QUAD,
        out_specs=vmem,
        scratch_shapes=[pltpu.VMEM((QUAD * plan.quarter + 2, 8, LANES), jnp.float32)],
        compiler_params=params(16),
        name="sketch_by_line",
    )(*from_vmem(*pieces))


def inverse_rows(plan, packed):
    row = row_of()
    lane = lane_of()
    packed = packed + roll(packed, 4, 0)
    entry = {}
    for d in range(3):
        for a in range(PROBES):
            b = (a + d) % PROBES
            if (max(a, b), min(a, b)) not in entry:
                chosen = jnp.where((row == a) & (lane == d), packed, 0.0)
                whole = jnp.sum(jnp.sum(chosen, axis=1, keepdims=True), axis=0, keepdims=True)
                entry[max(a, b), min(a, b)] = jnp.broadcast_to(whole, (8, LANES)) / plan.total
    low = {}
    inv = {}
    for j in range(PROBES):
        rest = entry[j, j]
        for m in range(j):
            rest = rest - low[j, m] * low[j, m]
        low[j, j] = jnp.sqrt(rest)
        inv[j, j] = 1.0 / low[j, j]
        for i in range(j + 1, PROBES):
            rest = entry[i, j]
            for m in range(j):
                rest = rest - low[i, m] * low[j, m]
            low[i, j] = rest * inv[j, j]
    for i in range(PROBES):
        for j in range(i):
            total = sum(low[i, m] * inv[m, j] for m in range(j, i))
            inv[i, j] = -total * inv[i, i]
    rows = []
    for d in range(PROBES):
        value = jnp.zeros((8, LANES), jnp.float32)
        for a in range(d, PROBES):
            value = jnp.where(row % 4 == a, inv[a, a - d], value)
        rows.append(value)
    return rows


def final_kernel(plan, sketch_ref, *rest):
    ins, basis_ref, coeffs_ref = rest[: plan.shards], rest[plan.shards], rest[plan.shards + 1]
    packed = sum(ref[plan.shard_lines] for ref in ins)
    rows = inverse_rows(plan, packed)

    def scaled(x):
        width = x.shape[1]
        return sum((rows[d][:, :width] * (roll(x, d, 0) if d else x)) for d in range(PROBES))

    for pair in range(plan.shard_lines // 2):
        two = [scaled(sum(ref[2 * pair + i] for ref in ins)) for i in range(2)]
        coeffs_ref[pl.ds(16 * pair, 16)] = jnp.concatenate(two, axis=0).astype(jnp.bfloat16)
    for line in range(plan.lines):
        for start in range(0, plan.group, LANES):
            width = min(LANES, plan.group - start)
            value = scaled(sketch_ref[line, :, pl.ds(start, width)])
            for part in range(2):
                basis_ref[line, part, :, pl.ds(start, width)] = value[4 * part : 4 * part + 4]


def finish(plan, sketch, pieces):
    vmem = pl.BlockSpec(memory_space=pltpu.VMEM)
    return pl.pallas_call(
        functools.partial(final_kernel, plan),
        out_shape=[
            jax.ShapeDtypeStruct((plan.lines, 2, PROBES, plan.group), jnp.float32),
            jax.ShapeDtypeStruct((plan.shard_lines * 8, LANES), jnp.bfloat16),
        ],
        in_specs=[vmem] * (1 + plan.shards),
        out_specs=[vmem] * 2,
        compiler_params=params(16),
        name="finish",
    )(*from_vmem(sketch, *pieces))


def trade(x, axis, size, k):
    return lax.ppermute(x, axis, [(i, i ^ k) for i in range(size)])


def sketch_and_adjoint(param, sensor, blocks, probes):
    lines, parts, group, nodes = blocks.shape
    plan = Plan(lines, parts, group, nodes, sensor)
    flat_blocks = blocks.transpose(0, 2, 1, 3).reshape(plan.rows, nodes)
    flat_probes = probes.reshape(lines * parts * PROBES, nodes)
    terms, kept, lhs = sketch_terms(plan, flat_blocks, flat_probes)
    total, kept[0] = own_terms(plan, flat_blocks, lhs)
    for k in REDUCE:
        total = total + trade(terms[k], "param", param, k)
    span = QUAD
    while span * 2 < param:
        total = total + trade(total, "param", param, span)
        span *= 2
    sums = [total] + ([trade(total, "param", param, span)] if span < param else [])
    own = add_with_gram(plan, *sums)
    pieces = [own] + [trade(own, "param", param, k) for k in range(1, QUAD)]
    adjoint = adjoint_terms(plan, (0, GATHER[0]), pieces, kept)
    adjoint = adjoint_terms(plan, GATHER[1:], pieces, kept, adjoint)
    gathered = [adjoint[0]] + [trade(adjoint[k], "sensor", sensor, k) for k in range(1, sensor)]
    sketch = sketch_by_line(plan, pieces)
    basis, coeffs = finish(plan, sketch, gathered)
    return basis, coeffs.reshape(plan.shard_lines, parts, PROBES, nodes)


def on_device(param, sensor, blocks, probes):
    return sketch_and_adjoint(param, sensor, blocks, probes)


def solution(mesh):
    param, sensor = mesh.shape["param"], mesh.shape["sensor"]
    assert param % QUAD == 0 and param & (param - 1) == 0 and sensor & (sensor - 1) == 0
    placed = (P(None, None, "sensor", "param"), P(None, None, None, "param"))
    return jax.shard_map(
        functools.partial(on_device, param, sensor),
        mesh=mesh,
        in_specs=placed,
        out_specs=(P(None, None, None, "sensor"), P("sensor", None, None, "param")),
        check_vma=False,
    )
```

```python
import functools

import jax
import jax.numpy as jnp
from jax import lax
from jax.experimental import pallas as pl
from jax.experimental.pallas import tpu as pltpu
from jax.sharding import PartitionSpec as P


LANES = 128
STEP = 2 * LANES
QUAD = 4
PROBES = 4
ARRIVALS = ((3,), (2,), (1,))
REDUCE, GATHER = (3, 2, 1), (3, 2, 1)
URGENCY = (0, 1, 1)
PIECES = 8
SPLITS = 3


MIB = 1 << 20


def in_vmem(shape, dtype):
    return pltpu.VMEM(shape, dtype)


def from_vmem(*arrays):
    return [pltpu.with_memory_space_constraint(x, pltpu.VMEM) for x in arrays]


def params(limit):
    return pltpu.CompilerParams(vmem_limit_bytes=limit * MIB)


def roll(x, shift, axis):
    return pltpu.roll(x, shift % x.shape[axis], axis)


def row_of(shape=(8, LANES)):
    return lax.broadcasted_iota(jnp.int32, shape, 0)


def lane_of(shape=(8, LANES)):
    return lax.broadcasted_iota(jnp.int32, shape, 1)


class Plan:
    def __init__(self, lines, parts, group, nodes, shards):
        self.lines, self.parts, self.group, self.nodes = lines, parts, group, nodes
        self.per_line = parts * group
        self.rows = lines * self.per_line
        self.steps = self.rows // STEP
        self.quarter = -(-self.steps // QUAD)
        self.shards = shards
        self.shard_lines = lines // shards
        self.total = parts * lines * group * shards
        assert parts == 2 and nodes == LANES and self.rows % STEP == 0 and self.per_line >= STEP
        assert lines % shards == 0 and self.steps > (QUAD - 1) * self.quarter


def first_line(plan, step):
    return (step * STEP) // plan.per_line


def quarter_copies(plan, k, blocks_ref, kept_ref, sems):
    first = (lax.axis_index("param") & (QUAD - 1) ^ k) * plan.quarter
    whole = plan.quarter - 1
    found = []
    for at, (start, count) in enumerate(((0, whole), (whole, 1))):
        source = jnp.minimum(first + start, plan.steps - count)
        found.append(
            pltpu.make_async_copy(
                blocks_ref.at[pl.ds(pl.multiple_of(source * STEP, STEP), count * STEP)],
                kept_ref.at[pl.ds(start * STEP, count * STEP)],
                sems.at[at],
            )
        )
    return found


def quarter_terms(plan, k, kept_ref, lhs_ref, out_ref):
    first = (lax.axis_index("param") & (QUAD - 1) ^ k) * plan.quarter
    low = row_of() < 4
    even = lane_of() % 2 == 0
    column = lane_of((8, STEP))

    def body(t, _):
        step = first + t
        line = first_line(plan, jnp.minimum(step, plan.steps - 1))
        probe = lhs_ref[pl.ds(pl.multiple_of(line * 8, 8), 16)].astype(jnp.bfloat16)
        block = kept_ref[pl.ds(pl.multiple_of(t * STEP, STEP), STEP)]
        both = lax.dot_general(probe, block, (((1,), (1,)), ((), ())), preferred_element_type=jnp.float32)
        place = column + step * STEP
        own = jnp.where(place < (line + 1) * plan.per_line, both[:8], both[8:])
        own = jnp.where(place < plan.rows, own, 0.0)
        left, right = own[:, :LANES], own[:, LANES:]
        direct = jnp.where(low, left, roll(right, 4, 0))
        crossed = jnp.where(low, roll(left, 4, 0), right)
        out_ref[t] = direct + jnp.where(even, -roll(crossed, -1, 1), roll(crossed, 1, 1))
        return 0

    lax.fori_loop(0, plan.quarter, body, 0, unroll=True)


def sent_kernel(plan, blocks_ref, probes_ref, *rest):
    count = QUAD - 1
    outs, kepts, (lhs_ref, held_ref, held_sem, sems) = rest[:count], rest[count : 2 * count], rest[2 * count :]
    load = pltpu.make_async_copy(probes_ref, held_ref, held_sem)
    load.start()
    copies = {k: quarter_copies(plan, k, blocks_ref, kept_ref, sems.at[k]) for k, kept_ref in zip(REDUCE, kepts)}
    for order, group in enumerate(ARRIVALS):
        for k in group:
            for copy in copies[k]:
                copy.start(priority=URGENCY[order])
    load.wait()
    held = plan.lines * 2 * PROBES
    lhs_ref[pl.ds(0, held)] = held_ref[...].astype(jnp.float32)
    lhs_ref[pl.ds(held, 8)] = jnp.zeros((8, LANES), jnp.float32)
    for group in ARRIVALS:
        for k in group:
            for copy in copies[k]:
                copy.wait()
        for k in group:
            at = REDUCE.index(k)
            quarter_terms(plan, k, kepts[at], lhs_ref, outs[at])


def own_kernel(plan, blocks_ref, lhs_ref, out_ref, kept_ref, sems):
    copies = quarter_copies(plan, 0, blocks_ref, kept_ref, sems)
    for copy in copies:
        copy.start()
    for copy in copies:
        copy.wait()
    quarter_terms(plan, 0, kept_ref, lhs_ref, out_ref)


def sketch_terms(plan, blocks, probes):
    piece = in_vmem((plan.quarter, 8, LANES), jnp.float32)
    kept = in_vmem((plan.quarter * STEP, LANES), jnp.bfloat16)
    lhs = in_vmem((plan.lines * 8 + 8, LANES), jnp.float32)
    vmem = pl.BlockSpec(memory_space=pltpu.VMEM)
    count = QUAD - 1
    out = pl.pallas_call(
        functools.partial(sent_kernel, plan),
        out_shape=[piece] * count + [kept] * count + [lhs],
        in_specs=[pl.BlockSpec(memory_space=pl.ANY)] * 2,
        out_specs=[vmem] * (2 * count + 1),
        scratch_shapes=[
            pltpu.VMEM((plan.lines * 8, LANES), jnp.bfloat16),
            pltpu.SemaphoreType.DMA(()),
            pltpu.SemaphoreType.DMA((QUAD, 2)),
        ],
        compiler_params=params(16),
        name="sent_terms",
    )(*[pltpu.with_memory_space_constraint(x, pltpu.HBM) for x in (blocks, probes)])
    return dict(zip(REDUCE, out[:count])), dict(zip(REDUCE, out[count:-1])), out[-1]


def own_terms(plan, blocks, lhs):
    vmem = pl.BlockSpec(memory_space=pltpu.VMEM)
    return pl.pallas_call(
        functools.partial(own_kernel, plan),
        out_shape=[
            in_vmem((plan.quarter, 8, LANES), jnp.float32),
            in_vmem((plan.quarter * STEP, LANES), jnp.bfloat16),
        ],
        in_specs=[pl.BlockSpec(memory_space=pl.ANY), vmem],
        out_specs=[vmem] * 2,
        scratch_shapes=[pltpu.SemaphoreType.DMA((2,))],
        compiler_params=params(16),
        name="own_terms",
    )(pltpu.with_memory_space_constraint(blocks, pltpu.HBM), *from_vmem(lhs))


def gram_kernel(plan, *refs):
    ins, out_ref = refs[:-1], refs[-1]
    row = row_of()
    lane = lane_of()
    sums = [jnp.zeros((8, LANES), jnp.float32) for _ in range(3)]
    for t in range(plan.quarter):
        x = ins[0][t]
        for other in ins[1:]:
            x = x + other[t]
        out_ref[t] = x
        for d in range(3):
            y = x if d == 0 else jnp.where(row % 4 + d < 4, roll(x, -d, 0), roll(x, 4 - d, 0))
            sums[d] = sums[d] + x * y
    packed = jnp.zeros((8, LANES), jnp.float32)
    for d in range(3):
        packed = jnp.where(lane == d, jnp.sum(sums[d], axis=1, keepdims=True), packed)
    out_ref[plan.quarter] = packed


def add_with_gram(plan, *pieces):
    vmem = pl.BlockSpec(memory_space=pltpu.VMEM)
    return pl.pallas_call(
        functools.partial(gram_kernel, plan),
        out_shape=in_vmem((plan.quarter + 1, 8, LANES), jnp.float32),
        in_specs=[vmem] * len(pieces),
        out_specs=vmem,
        compiler_params=params(16),
        name="add_with_gram",
    )(*from_vmem(*pieces))


def adjoint_kernel(plan, distances, follows, last, *refs):
    count = len(distances)
    ins, kepts, rest = refs[:count], refs[count : 2 * count], refs[2 * count :]
    earlier = rest[0] if follows else None
    acc_ref = rest[-1]
    param = lax.axis_index("param")
    low = row_of() < 4
    even = lane_of() % 2 == 0
    column = lane_of((8, STEP))
    if follows and not last:
        acc_ref[...] = earlier[...]
    else:
        acc_ref[...] = jnp.zeros(acc_ref.shape, jnp.float32)
    for k, in_ref, kept_ref in zip(distances, ins, kepts):
        first = (param & (QUAD - 1) ^ k) * plan.quarter

        def body(t, _, first=first, in_ref=in_ref, kept_ref=kept_ref):
            step = jnp.minimum(first + t, plan.steps - 1)
            line = first_line(plan, step)
            x = in_ref[t]
            y = jnp.where(even, roll(x, -1, 1), -roll(x, 1, 1))
            left = jnp.where(low, x, roll(y, 4, 0))
            right = jnp.where(low, roll(x, 4, 0), y)
            value = jnp.concatenate([left, right], axis=1)
            mine = column + step * STEP < (line + 1) * plan.per_line
            terms = []
            for _ in range(SPLITS):
                term = value.astype(jnp.bfloat16).astype(jnp.float32)
                terms.append(jnp.where(mine, term, 0.0))
                terms.append(jnp.where(mine, 0.0, term))
                value = value - term
            lhs = jnp.concatenate(terms, axis=0).astype(jnp.bfloat16)
            block = kept_ref[pl.ds(pl.multiple_of(t * STEP, STEP), STEP)]
            got = jnp.dot(lhs, block, preferred_element_type=jnp.float32)
            here = sum(got[16 * i : 16 * i + 8] for i in range(SPLITS))
            after = sum(got[16 * i + 8 : 16 * i + 16] for i in range(SPLITS))
            acc_ref[line] = acc_ref[line] + here
            acc_ref[line + 1] = acc_ref[line + 1] + after
            return 0

        lax.fori_loop(0, plan.quarter, body, 0, unroll=True)
    packed = sum(ref[plan.quarter] for ref in ins)
    if follows:
        packed = packed + earlier[plan.lines]
    if not last:
        acc_ref[plan.lines] = packed
        return
    spot = lax.axis_index("sensor")
    for k, out_ref in enumerate(rest[1:-1]):
        lines = pl.ds((spot ^ k) * plan.shard_lines, plan.shard_lines)
        out_ref[pl.ds(0, plan.shard_lines)] = acc_ref[lines] + earlier[lines]
        out_ref[plan.shard_lines] = packed


def adjoint_terms(plan, distances, pieces, kept, earlier=None, last=False):
    vmem = pl.BlockSpec(memory_space=pltpu.VMEM)
    whole = in_vmem((plan.lines + 1, 8, LANES), jnp.float32)
    shard = in_vmem((plan.shard_lines + 1, 8, LANES), jnp.float32)
    given = [pieces[k] for k in distances] + [kept[k] for k in distances]
    if earlier is not None:
        given.append(earlier)
    return pl.pallas_call(
        functools.partial(adjoint_kernel, plan, distances, earlier is not None, last),
        out_shape=[shard] * plan.shards if last else whole,
        in_specs=[vmem] * len(given),
        out_specs=[vmem] * plan.shards if last else vmem,
        scratch_shapes=[whole] if last else [],
        compiler_params=params(16),
        name="adjoint_last" if last else "adjoint_part",
    )(*from_vmem(*given))


def by_line_kernel(plan, *rest):
    ins, out_ref, flat_ref = rest[:QUAD], rest[QUAD], rest[QUAD + 1]
    me = lax.axis_index("param") & (QUAD - 1)
    lane = lane_of()
    half = LANES // 2
    stay = (row_of() < 4) == (lane < half)
    source = jnp.where(lane < half, 2 * lane, 2 * lane - (LANES - 1))
    for k in range(QUAD):
        first = (me ^ k) * plan.quarter
        for t in range(plan.quarter):
            split = jnp.take_along_axis(ins[k][t], source, axis=1)
            flat_ref[first + t] = jnp.where(stay, split, roll(roll(split, 4, 0), half, 1))
    tiles = -(-plan.group // LANES)
    for line in range(plan.lines):
        tile, shift = divmod(line * plan.group, LANES)
        turned = [roll(flat_ref[tile + i], -shift, 1) for i in range(tiles + 1)]
        for i in range(tiles):
            width = min(LANES, plan.group - i * LANES)
            part = jnp.where(lane < LANES - shift, turned[i], turned[i + 1])
            out_ref[line, :, pl.ds(i * LANES, width)] = part[:, :width]


def sketch_by_line(plan, pieces):
    vmem = pl.BlockSpec(memory_space=pltpu.VMEM)
    return pl.pallas_call(
        functools.partial(by_line_kernel, plan),
        out_shape=in_vmem((plan.lines, 8, plan.group), jnp.float32),
        in_specs=[vmem] * QUAD,
        out_specs=vmem,
        scratch_shapes=[pltpu.VMEM((QUAD * plan.quarter + 2, 8, LANES), jnp.float32)],
        compiler_params=params(16),
        name="sketch_by_line",
    )(*from_vmem(*pieces))


def inverse_rows(plan, packed):
    row = row_of()
    lane = lane_of()
    packed = packed + roll(packed, 4, 0)
    entry = {}
    for d in range(3):
        for a in range(PROBES):
            b = (a + d) % PROBES
            if (max(a, b), min(a, b)) not in entry:
                chosen = jnp.where((row == a) & (lane == d), packed, 0.0)
                whole = jnp.sum(jnp.sum(chosen, axis=1, keepdims=True), axis=0, keepdims=True)
                entry[max(a, b), min(a, b)] = jnp.broadcast_to(whole, (8, LANES)) / plan.total
    low = {}
    inv = {}
    for j in range(PROBES):
        rest = entry[j, j]
        for m in range(j):
            rest = rest - low[j, m] * low[j, m]
        low[j, j] = jnp.sqrt(rest)
        inv[j, j] = 1.0 / low[j, j]
        for i in range(j + 1, PROBES):
            rest = entry[i, j]
            for m in range(j):
                rest = rest - low[i, m] * low[j, m]
            low[i, j] = rest * inv[j, j]
    for i in range(PROBES):
        for j in range(i):
            total = sum(low[i, m] * inv[m, j] for m in range(j, i))
            inv[i, j] = -total * inv[i, i]
    rows = []
    for d in range(PROBES):
        value = jnp.zeros((8, LANES), jnp.float32)
        for a in range(d, PROBES):
            value = jnp.where(row % 4 == a, inv[a, a - d], value)
        rows.append(value)
    return rows


def final_kernel(plan, sketch_ref, *rest):
    ins, (basis_out, coeffs_out, basis_ref, coeffs_ref, sems) = rest[: plan.shards], rest[plan.shards :]
    packed = sum(ref[plan.shard_lines] for ref in ins)
    rows = inverse_rows(plan, packed)

    def scaled(x):
        width = x.shape[1]
        return sum((rows[d][:, :width] * (roll(x, d, 0) if d else x)) for d in range(PROBES))

    copies = []
    for at in range(PIECES):
        low, high = at * plan.lines // PIECES, (at + 1) * plan.lines // PIECES
        for line in range(low, high):
            for start in range(0, plan.group, LANES):
                width = min(LANES, plan.group - start)
                value = scaled(sketch_ref[line, :, pl.ds(start, width)])
                for part in range(2):
                    basis_ref[line, part, :, pl.ds(start, width)] = value[4 * part : 4 * part + 4]
        made = pl.ds(low, high - low)
        copies.append(pltpu.make_async_copy(basis_ref.at[made], basis_out.at[made], sems.at[at]))
        copies[-1].start()
    for pair in range(plan.shard_lines // 2):
        two = [scaled(sum(ref[2 * pair + i] for ref in ins)) for i in range(2)]
        coeffs_ref[pl.ds(16 * pair, 16)] = jnp.concatenate(two, axis=0).astype(jnp.bfloat16)
    copies.append(pltpu.make_async_copy(coeffs_ref, coeffs_out, sems.at[PIECES]))
    copies[-1].start()
    for copy in copies:
        copy.wait()


def finish(plan, sketch, pieces):
    vmem = pl.BlockSpec(memory_space=pltpu.VMEM)
    basis = (plan.lines, 2, PROBES, plan.group)
    coeffs = (plan.shard_lines * 8, LANES)
    return pl.pallas_call(
        functools.partial(final_kernel, plan),
        out_shape=[jax.ShapeDtypeStruct(basis, jnp.float32), jax.ShapeDtypeStruct(coeffs, jnp.bfloat16)],
        in_specs=[vmem] * (1 + plan.shards),
        out_specs=[pl.BlockSpec(memory_space=pltpu.HBM)] * 2,
        scratch_shapes=[
            pltpu.VMEM(basis, jnp.float32),
            pltpu.VMEM(coeffs, jnp.bfloat16),
            pltpu.SemaphoreType.DMA((PIECES + 1,)),
        ],
        compiler_params=params(16),
        name="finish",
    )(*from_vmem(sketch, *pieces))


def trade(x, axis, size, k):
    return lax.ppermute(x, axis, [(i, i ^ k) for i in range(size)])


def sketch_and_adjoint(param, sensor, blocks, probes):
    lines, parts, group, nodes = blocks.shape
    plan = Plan(lines, parts, group, nodes, sensor)
    flat_blocks = blocks.transpose(0, 2, 1, 3).reshape(plan.rows, nodes)
    flat_probes = probes.reshape(lines * parts * PROBES, nodes)
    terms, kept, lhs = sketch_terms(plan, flat_blocks, flat_probes)
    total, kept[0] = own_terms(plan, flat_blocks, lhs)
    for k in REDUCE:
        total = total + trade(terms[k], "param", param, k)
    span = QUAD
    while span * 2 < param:
        total = total + trade(total, "param", param, span)
        span *= 2
    sums = [total] + ([trade(total, "param", param, span)] if span < param else [])
    own = add_with_gram(plan, *sums)
    pieces = [own] + [trade(own, "param", param, k) for k in range(1, QUAD)]
    adjoint = adjoint_terms(plan, (0,), pieces, kept)
    adjoint = adjoint_terms(plan, GATHER[:-1], pieces, kept, adjoint)
    adjoint = adjoint_terms(plan, GATHER[-1:], pieces, kept, adjoint, True)
    gathered = [adjoint[0]] + [trade(adjoint[k], "sensor", sensor, k) for k in range(1, sensor)]
    sketch = sketch_by_line(plan, pieces)
    basis, coeffs = finish(plan, sketch, gathered)
    return basis, coeffs.reshape(plan.shard_lines, parts, PROBES, nodes)


def on_device(param, sensor, blocks, probes):
    return sketch_and_adjoint(param, sensor, blocks, probes)


def solution(mesh):
    param, sensor = mesh.shape["param"], mesh.shape["sensor"]
    assert param % QUAD == 0 and param & (param - 1) == 0 and sensor & (sensor - 1) == 0
    placed = (P(None, None, "sensor", "param"), P(None, None, None, "param"))
    return jax.shard_map(
        functools.partial(on_device, param, sensor),
        mesh=mesh,
        in_specs=placed,
        out_specs=(P(None, None, None, "sensor"), P("sensor", None, None, "param")),
        check_vma=False,
    )
```

```python
import functools

import jax
import jax.numpy as jnp
from jax import lax
from jax.experimental import pallas as pl
from jax.experimental.pallas import tpu as pltpu
from jax.sharding import PartitionSpec as P


LANES = 128
STEP = 2 * LANES
QUAD = 4
PROBES = 4
ARRIVALS = ((3,), (2,), (1,))
REDUCE, GATHER = (3, 2, 1), (3, 2, 1)
URGENCY = (0, 1, 1)
PIECES = 8
SPLITS = 3


MIB = 1 << 20


def in_vmem(shape, dtype):
    return pltpu.VMEM(shape, dtype)


def from_vmem(*arrays):
    return [pltpu.with_memory_space_constraint(x, pltpu.VMEM) for x in arrays]


def params(limit):
    return pltpu.CompilerParams(vmem_limit_bytes=limit * MIB)


def roll(x, shift, axis):
    return pltpu.roll(x, shift % x.shape[axis], axis)


def row_of(shape=(8, LANES)):
    return lax.broadcasted_iota(jnp.int32, shape, 0)


def lane_of(shape=(8, LANES)):
    return lax.broadcasted_iota(jnp.int32, shape, 1)


class Plan:
    def __init__(self, lines, parts, group, nodes, shards):
        self.lines, self.parts, self.group, self.nodes = lines, parts, group, nodes
        self.per_line = parts * group
        self.rows = lines * self.per_line
        self.steps = self.rows // STEP
        self.quarter = -(-self.steps // QUAD)
        self.shards = shards
        self.shard_lines = lines // shards
        self.total = parts * lines * group * shards
        assert parts == 2 and nodes == LANES and self.rows % STEP == 0 and self.per_line >= STEP
        assert lines % shards == 0 and self.steps > (QUAD - 1) * self.quarter


def first_line(plan, step):
    return (step * STEP) // plan.per_line


def quarter_copies(plan, k, blocks_ref, kept_ref, sems):
    first = (lax.axis_index("param") & (QUAD - 1) ^ k) * plan.quarter
    whole = plan.quarter - 1
    found = []
    for at, (start, count) in enumerate(((0, whole), (whole, 1))):
        source = jnp.minimum(first + start, plan.steps - count)
        found.append(
            pltpu.make_async_copy(
                blocks_ref.at[pl.ds(pl.multiple_of(source * STEP, STEP), count * STEP)],
                kept_ref.at[pl.ds(start * STEP, count * STEP)],
                sems.at[at],
            )
        )
    return found


def quarter_terms(plan, k, kept_ref, lhs_ref, out_ref):
    first = (lax.axis_index("param") & (QUAD - 1) ^ k) * plan.quarter
    low = row_of() < 4
    even = lane_of() % 2 == 0
    column = lane_of((8, STEP))

    def body(t, _):
        step = first + t
        line = first_line(plan, jnp.minimum(step, plan.steps - 1))
        probe = lhs_ref[pl.ds(pl.multiple_of(line * 8, 8), 16)].astype(jnp.bfloat16)
        block = kept_ref[pl.ds(pl.multiple_of(t * STEP, STEP), STEP)]
        both = lax.dot_general(probe, block, (((1,), (1,)), ((), ())), preferred_element_type=jnp.float32)
        place = column + step * STEP
        own = jnp.where(place < (line + 1) * plan.per_line, both[:8], both[8:])
        own = jnp.where(place < plan.rows, own, 0.0)
        left, right = own[:, :LANES], own[:, LANES:]
        direct = jnp.where(low, left, roll(right, 4, 0))
        crossed = jnp.where(low, roll(left, 4, 0), right)
        out_ref[t] = direct + jnp.where(even, -roll(crossed, -1, 1), roll(crossed, 1, 1))
        return 0

    lax.fori_loop(0, plan.quarter, body, 0, unroll=True)


def sent_kernel(plan, blocks_ref, probes_ref, *rest):
    count = QUAD - 1
    outs, kepts, (lhs_ref, held_ref, held_sem, sems) = rest[:count], rest[count : 2 * count], rest[2 * count :]
    load = pltpu.make_async_copy(probes_ref, held_ref, held_sem)
    load.start()
    copies = {k: quarter_copies(plan, k, blocks_ref, kept_ref, sems.at[k]) for k, kept_ref in zip(REDUCE, kepts)}
    for order, group in enumerate(ARRIVALS):
        for k in group:
            for copy in copies[k]:
                copy.start(priority=URGENCY[order])
    load.wait()
    held = plan.lines * 2 * PROBES
    lhs_ref[pl.ds(0, held)] = held_ref[...].astype(jnp.float32)
    lhs_ref[pl.ds(held, 8)] = jnp.zeros((8, LANES), jnp.float32)
    for group in ARRIVALS:
        for k in group:
            for copy in copies[k]:
                copy.wait()
        for k in group:
            at = REDUCE.index(k)
            quarter_terms(plan, k, kepts[at], lhs_ref, outs[at])


def own_kernel(plan, blocks_ref, lhs_ref, out_ref, kept_ref, sems):
    copies = quarter_copies(plan, 0, blocks_ref, kept_ref, sems)
    for copy in copies:
        copy.start()
    for copy in copies:
        copy.wait()
    quarter_terms(plan, 0, kept_ref, lhs_ref, out_ref)


def sketch_terms(plan, blocks, probes):
    piece = in_vmem((plan.quarter, 8, LANES), jnp.float32)
    kept = in_vmem((plan.quarter * STEP, LANES), jnp.bfloat16)
    lhs = in_vmem((plan.lines * 8 + 8, LANES), jnp.float32)
    vmem = pl.BlockSpec(memory_space=pltpu.VMEM)
    count = QUAD - 1
    out = pl.pallas_call(
        functools.partial(sent_kernel, plan),
        out_shape=[piece] * count + [kept] * count + [lhs],
        in_specs=[pl.BlockSpec(memory_space=pl.ANY)] * 2,
        out_specs=[vmem] * (2 * count + 1),
        scratch_shapes=[
            pltpu.VMEM((plan.lines * 8, LANES), jnp.bfloat16),
            pltpu.SemaphoreType.DMA(()),
            pltpu.SemaphoreType.DMA((QUAD, 2)),
        ],
        compiler_params=params(16),
        name="sent_terms",
    )(*[pltpu.with_memory_space_constraint(x, pltpu.HBM) for x in (blocks, probes)])
    return dict(zip(REDUCE, out[:count])), dict(zip(REDUCE, out[count:-1])), out[-1]


def own_terms(plan, blocks, lhs):
    vmem = pl.BlockSpec(memory_space=pltpu.VMEM)
    return pl.pallas_call(
        functools.partial(own_kernel, plan),
        out_shape=[
            in_vmem((plan.quarter, 8, LANES), jnp.float32),
            in_vmem((plan.quarter * STEP, LANES), jnp.bfloat16),
        ],
        in_specs=[pl.BlockSpec(memory_space=pl.ANY), vmem],
        out_specs=[vmem] * 2,
        scratch_shapes=[pltpu.SemaphoreType.DMA((2,))],
        compiler_params=params(16),
        name="own_terms",
    )(pltpu.with_memory_space_constraint(blocks, pltpu.HBM), *from_vmem(lhs))


def gram_terms(plan, ins):
    row = row_of()
    lane = lane_of()
    sums = [jnp.zeros((8, LANES), jnp.float32) for _ in range(3)]
    for in_ref in ins:
        for t in range(plan.quarter):
            x = in_ref[t]
            for d in range(3):
                y = x if d == 0 else jnp.where(row % 4 + d < 4, roll(x, -d, 0), roll(x, 4 - d, 0))
                sums[d] = sums[d] + x * y
    packed = jnp.zeros((8, LANES), jnp.float32)
    for d in range(3):
        packed = jnp.where(lane == d, jnp.sum(sums[d], axis=1, keepdims=True), packed)
    return packed


def adjoint_kernel(plan, distances, follows, last, *refs):
    count = len(distances)
    ins, kepts, rest = refs[:count], refs[count : 2 * count], refs[2 * count :]
    earlier = rest[0] if follows else None
    acc_ref = rest[-1]
    param = lax.axis_index("param")
    low = row_of() < 4
    even = lane_of() % 2 == 0
    column = lane_of((8, STEP))
    if follows and not last:
        acc_ref[...] = earlier[...]
    else:
        acc_ref[...] = jnp.zeros(acc_ref.shape, jnp.float32)
    for k, in_ref, kept_ref in zip(distances, ins, kepts):
        first = (param & (QUAD - 1) ^ k) * plan.quarter

        def body(t, _, first=first, in_ref=in_ref, kept_ref=kept_ref):
            step = jnp.minimum(first + t, plan.steps - 1)
            line = first_line(plan, step)
            x = in_ref[t]
            y = jnp.where(even, roll(x, -1, 1), -roll(x, 1, 1))
            left = jnp.where(low, x, roll(y, 4, 0))
            right = jnp.where(low, roll(x, 4, 0), y)
            value = jnp.concatenate([left, right], axis=1)
            mine = column + step * STEP < (line + 1) * plan.per_line
            terms = []
            for _ in range(SPLITS):
                term = value.astype(jnp.bfloat16).astype(jnp.float32)
                terms.append(jnp.where(mine, term, 0.0))
                terms.append(jnp.where(mine, 0.0, term))
                value = value - term
            lhs = jnp.concatenate(terms, axis=0).astype(jnp.bfloat16)
            block = kept_ref[pl.ds(pl.multiple_of(t * STEP, STEP), STEP)]
            got = jnp.dot(lhs, block, preferred_element_type=jnp.float32)
            here = sum(got[16 * i : 16 * i + 8] for i in range(SPLITS))
            after = sum(got[16 * i + 8 : 16 * i + 16] for i in range(SPLITS))
            acc_ref[line] = acc_ref[line] + here
            acc_ref[line + 1] = acc_ref[line + 1] + after
            return 0

        lax.fori_loop(0, plan.quarter, body, 0, unroll=True)
    packed = gram_terms(plan, ins)
    if follows:
        packed = packed + earlier[plan.lines]
    if not last:
        acc_ref[plan.lines] = packed
        return
    spot = lax.axis_index("sensor")
    for k, out_ref in enumerate(rest[1:-1]):
        lines = pl.ds((spot ^ k) * plan.shard_lines, plan.shard_lines)
        out_ref[pl.ds(0, plan.shard_lines)] = acc_ref[lines] + earlier[lines]
        out_ref[plan.shard_lines] = packed


def adjoint_terms(plan, distances, pieces, kept, earlier=None, last=False):
    vmem = pl.BlockSpec(memory_space=pltpu.VMEM)
    whole = in_vmem((plan.lines + 1, 8, LANES), jnp.float32)
    shard = in_vmem((plan.shard_lines + 1, 8, LANES), jnp.float32)
    given = [pieces[k] for k in distances] + [kept[k] for k in distances]
    if earlier is not None:
        given.append(earlier)
    return pl.pallas_call(
        functools.partial(adjoint_kernel, plan, distances, earlier is not None, last),
        out_shape=[shard] * plan.shards if last else whole,
        in_specs=[vmem] * len(given),
        out_specs=[vmem] * plan.shards if last else vmem,
        scratch_shapes=[whole] if last else [],
        compiler_params=params(16),
        name="adjoint_last" if last else "adjoint_part",
    )(*from_vmem(*given))


def by_line_kernel(plan, *rest):
    ins, out_ref, flat_ref = rest[:QUAD], rest[QUAD], rest[QUAD + 1]
    me = lax.axis_index("param") & (QUAD - 1)
    lane = lane_of()
    half = LANES // 2
    stay = (row_of() < 4) == (lane < half)
    source = jnp.where(lane < half, 2 * lane, 2 * lane - (LANES - 1))
    for k in range(QUAD):
        first = (me ^ k) * plan.quarter
        for t in range(plan.quarter):
            split = jnp.take_along_axis(ins[k][t], source, axis=1)
            flat_ref[first + t] = jnp.where(stay, split, roll(roll(split, 4, 0), half, 1))
    tiles = -(-plan.group // LANES)
    for line in range(plan.lines):
        tile, shift = divmod(line * plan.group, LANES)
        turned = [roll(flat_ref[tile + i], -shift, 1) for i in range(tiles + 1)]
        for i in range(tiles):
            width = min(LANES, plan.group - i * LANES)
            part = jnp.where(lane < LANES - shift, turned[i], turned[i + 1])
            out_ref[line, :, pl.ds(i * LANES, width)] = part[:, :width]


def sketch_by_line(plan, pieces):
    vmem = pl.BlockSpec(memory_space=pltpu.VMEM)
    return pl.pallas_call(
        functools.partial(by_line_kernel, plan),
        out_shape=in_vmem((plan.lines, 8, plan.group), jnp.float32),
        in_specs=[vmem] * QUAD,
        out_specs=vmem,
        scratch_shapes=[pltpu.VMEM((QUAD * plan.quarter + 2, 8, LANES), jnp.float32)],
        compiler_params=params(16),
        name="sketch_by_line",
    )(*from_vmem(*pieces))


def inverse_rows(plan, packed):
    row = row_of()
    lane = lane_of()
    packed = packed + roll(packed, 4, 0)
    entry = {}
    for d in range(3):
        for a in range(PROBES):
            b = (a + d) % PROBES
            if (max(a, b), min(a, b)) not in entry:
                chosen = jnp.where((row == a) & (lane == d), packed, 0.0)
                whole = jnp.sum(jnp.sum(chosen, axis=1, keepdims=True), axis=0, keepdims=True)
                entry[max(a, b), min(a, b)] = jnp.broadcast_to(whole, (8, LANES)) / plan.total
    low = {}
    inv = {}
    for j in range(PROBES):
        rest = entry[j, j]
        for m in range(j):
            rest = rest - low[j, m] * low[j, m]
        low[j, j] = jnp.sqrt(rest)
        inv[j, j] = 1.0 / low[j, j]
        for i in range(j + 1, PROBES):
            rest = entry[i, j]
            for m in range(j):
                rest = rest - low[i, m] * low[j, m]
            low[i, j] = rest * inv[j, j]
    for i in range(PROBES):
        for j in range(i):
            total = sum(low[i, m] * inv[m, j] for m in range(j, i))
            inv[i, j] = -total * inv[i, i]
    rows = []
    for d in range(PROBES):
        value = jnp.zeros((8, LANES), jnp.float32)
        for a in range(d, PROBES):
            value = jnp.where(row % 4 == a, inv[a, a - d], value)
        rows.append(value)
    return rows


def final_kernel(plan, sketch_ref, *rest):
    ins, (basis_out, coeffs_out, basis_ref, coeffs_ref, sems) = rest[: plan.shards], rest[plan.shards :]
    packed = sum(ref[plan.shard_lines] for ref in ins)
    rows = inverse_rows(plan, packed)

    def scaled(x):
        width = x.shape[1]
        return sum((rows[d][:, :width] * (roll(x, d, 0) if d else x)) for d in range(PROBES))

    copies = []
    for at in range(PIECES):
        low, high = at * plan.lines // PIECES, (at + 1) * plan.lines // PIECES
        for line in range(low, high):
            for start in range(0, plan.group, LANES):
                width = min(LANES, plan.group - start)
                value = scaled(sketch_ref[line, :, pl.ds(start, width)])
                for part in range(2):
                    basis_ref[line, part, :, pl.ds(start, width)] = value[4 * part : 4 * part + 4]
        made = pl.ds(low, high - low)
        copies.append(pltpu.make_async_copy(basis_ref.at[made], basis_out.at[made], sems.at[at]))
        copies[-1].start()
    for pair in range(plan.shard_lines // 2):
        two = [scaled(sum(ref[2 * pair + i] for ref in ins)) for i in range(2)]
        coeffs_ref[pl.ds(16 * pair, 16)] = jnp.concatenate(two, axis=0).astype(jnp.bfloat16)
    copies.append(pltpu.make_async_copy(coeffs_ref, coeffs_out, sems.at[PIECES]))
    copies[-1].start()
    for copy in copies:
        copy.wait()


def finish(plan, sketch, pieces):
    vmem = pl.BlockSpec(memory_space=pltpu.VMEM)
    basis = (plan.lines, 2, PROBES, plan.group)
    coeffs = (plan.shard_lines * 8, LANES)
    return pl.pallas_call(
        functools.partial(final_kernel, plan),
        out_shape=[jax.ShapeDtypeStruct(basis, jnp.float32), jax.ShapeDtypeStruct(coeffs, jnp.bfloat16)],
        in_specs=[vmem] * (1 + plan.shards),
        out_specs=[pl.BlockSpec(memory_space=pltpu.HBM)] * 2,
        scratch_shapes=[
            pltpu.VMEM(basis, jnp.float32),
            pltpu.VMEM(coeffs, jnp.bfloat16),
            pltpu.SemaphoreType.DMA((PIECES + 1,)),
        ],
        compiler_params=params(16),
        name="finish",
    )(*from_vmem(sketch, *pieces))


def trade(x, axis, size, k):
    return lax.ppermute(x, axis, [(i, i ^ k) for i in range(size)])


def sketch_and_adjoint(param, sensor, blocks, probes):
    lines, parts, group, nodes = blocks.shape
    plan = Plan(lines, parts, group, nodes, sensor)
    flat_blocks = blocks.transpose(0, 2, 1, 3).reshape(plan.rows, nodes)
    flat_probes = probes.reshape(lines * parts * PROBES, nodes)
    terms, kept, lhs = sketch_terms(plan, flat_blocks, flat_probes)
    total, kept[0] = own_terms(plan, flat_blocks, lhs)
    for k in REDUCE:
        total = total + trade(terms[k], "param", param, k)
    span = QUAD
    while span * 2 < param:
        total = total + trade(total, "param", param, span)
        span *= 2
    sums = [total] + ([trade(total, "param", param, span)] if span < param else [])
    own = sum(sums)
    pieces = [own] + [trade(own, "param", param, k) for k in range(1, QUAD)]
    adjoint = adjoint_terms(plan, (0,), pieces, kept)
    adjoint = adjoint_terms(plan, GATHER[:-1], pieces, kept, adjoint)
    adjoint = adjoint_terms(plan, GATHER[-1:], pieces, kept, adjoint, True)
    gathered = [adjoint[0]] + [trade(adjoint[k], "sensor", sensor, k) for k in range(1, sensor)]
    sketch = sketch_by_line(plan, pieces)
    basis, coeffs = finish(plan, sketch, gathered)
    return basis, coeffs.reshape(plan.shard_lines, parts, PROBES, nodes)


def on_device(param, sensor, blocks, probes):
    return sketch_and_adjoint(param, sensor, blocks, probes)


def solution(mesh):
    param, sensor = mesh.shape["param"], mesh.shape["sensor"]
    assert param % QUAD == 0 and param & (param - 1) == 0 and sensor & (sensor - 1) == 0
    placed = (P(None, None, "sensor", "param"), P(None, None, None, "param"))
    return jax.shard_map(
        functools.partial(on_device, param, sensor),
        mesh=mesh,
        in_specs=placed,
        out_specs=(P(None, None, None, "sensor"), P("sensor", None, None, "param")),
        check_vma=False,
    )
```

```python
import functools

import jax
import jax.numpy as jnp
from jax import lax
from jax.experimental import pallas as pl
from jax.experimental.pallas import tpu as pltpu
from jax.sharding import PartitionSpec as P


LANES = 128
STEP = 2 * LANES
QUAD = 4
PROBES = 4
ARRIVALS = ((3,), (2, 1))
REDUCE, GATHER = (3, 2, 1), (3, 2, 1)
URGENCY = (0, 1, 1)
PIECES = 2
SPLITS = 3


MIB = 1 << 20


def in_vmem(shape, dtype):
    return pltpu.VMEM(shape, dtype)


def from_vmem(*arrays):
    return [pltpu.with_memory_space_constraint(x, pltpu.VMEM) for x in arrays]


def params(limit):
    return pltpu.CompilerParams(vmem_limit_bytes=limit * MIB)


def roll(x, shift, axis):
    return pltpu.roll(x, shift % x.shape[axis], axis)


def row_of(shape=(8, LANES)):
    return lax.broadcasted_iota(jnp.int32, shape, 0)


def lane_of(shape=(8, LANES)):
    return lax.broadcasted_iota(jnp.int32, shape, 1)


class Plan:
    def __init__(self, lines, parts, group, nodes, shards):
        self.lines, self.parts, self.group, self.nodes = lines, parts, group, nodes
        self.per_line = parts * group
        self.rows = lines * self.per_line
        self.steps = self.rows // STEP
        self.quarter = -(-self.steps // QUAD)
        self.shards = shards
        self.shard_lines = lines // shards
        self.total = parts * lines * group * shards
        assert parts == 2 and nodes == LANES and self.rows % STEP == 0 and self.per_line >= STEP
        assert lines % shards == 0 and self.steps > (QUAD - 1) * self.quarter


def first_line(plan, step):
    return (step * STEP) // plan.per_line


def quarter_copies(plan, k, blocks_ref, kept_ref, sems):
    first = (lax.axis_index("param") & (QUAD - 1) ^ k) * plan.quarter
    whole = plan.quarter - 1
    found = []
    for at, (start, count) in enumerate(((0, whole), (whole, 1))):
        source = jnp.minimum(first + start, plan.steps - count)
        found.append(
            pltpu.make_async_copy(
                blocks_ref.at[pl.ds(pl.multiple_of(source * STEP, STEP), count * STEP)],
                kept_ref.at[pl.ds(start * STEP, count * STEP)],
                sems.at[at],
            )
        )
    return found


def quarter_terms(plan, k, kept_ref, lhs_ref, out_ref):
    first = (lax.axis_index("param") & (QUAD - 1) ^ k) * plan.quarter
    low = row_of() < 4
    even = lane_of() % 2 == 0
    column = lane_of((8, STEP))

    def body(t, _):
        step = first + t
        line = first_line(plan, jnp.minimum(step, plan.steps - 1))
        probe = lhs_ref[pl.ds(pl.multiple_of(line * 8, 8), 16)].astype(jnp.bfloat16)
        block = kept_ref[pl.ds(pl.multiple_of(t * STEP, STEP), STEP)]
        both = lax.dot_general(probe, block, (((1,), (1,)), ((), ())), preferred_element_type=jnp.float32)
        place = column + step * STEP
        own = jnp.where(place < (line + 1) * plan.per_line, both[:8], both[8:])
        own = jnp.where(place < plan.rows, own, 0.0)
        left, right = own[:, :LANES], own[:, LANES:]
        direct = jnp.where(low, left, roll(right, 4, 0))
        crossed = jnp.where(low, roll(left, 4, 0), right)
        out_ref[t] = direct + jnp.where(even, -roll(crossed, -1, 1), roll(crossed, 1, 1))
        return 0

    lax.fori_loop(0, plan.quarter, body, 0, unroll=True)


def sent_kernel(plan, blocks_ref, probes_ref, *rest):
    count = QUAD - 1
    outs, kepts, (lhs_ref, held_ref, held_sem, sems) = rest[:count], rest[count : 2 * count], rest[2 * count :]
    load = pltpu.make_async_copy(probes_ref, held_ref, held_sem)
    load.start()
    copies = {k: quarter_copies(plan, k, blocks_ref, kept_ref, sems.at[k]) for k, kept_ref in zip(REDUCE, kepts)}
    for order, group in enumerate(ARRIVALS):
        for k in group:
            for copy in copies[k]:
                copy.start(priority=URGENCY[order])
    load.wait()
    held = plan.lines * 2 * PROBES
    lhs_ref[pl.ds(0, held)] = held_ref[...].astype(jnp.float32)
    lhs_ref[pl.ds(held, 8)] = jnp.zeros((8, LANES), jnp.float32)
    for group in ARRIVALS:
        for k in group:
            for copy in copies[k]:
                copy.wait()
        for k in group:
            at = REDUCE.index(k)
            quarter_terms(plan, k, kepts[at], lhs_ref, outs[at])


def own_kernel(plan, blocks_ref, lhs_ref, out_ref, kept_ref, sems):
    copies = quarter_copies(plan, 0, blocks_ref, kept_ref, sems)
    for copy in copies:
        copy.start()
    for copy in copies:
        copy.wait()
    quarter_terms(plan, 0, kept_ref, lhs_ref, out_ref)


def sketch_terms(plan, blocks, probes):
    piece = in_vmem((plan.quarter, 8, LANES), jnp.float32)
    kept = in_vmem((plan.quarter * STEP, LANES), jnp.bfloat16)
    lhs = in_vmem((plan.lines * 8 + 8, LANES), jnp.float32)
    vmem = pl.BlockSpec(memory_space=pltpu.VMEM)
    count = QUAD - 1
    out = pl.pallas_call(
        functools.partial(sent_kernel, plan),
        out_shape=[piece] * count + [kept] * count + [lhs],
        in_specs=[pl.BlockSpec(memory_space=pl.ANY)] * 2,
        out_specs=[vmem] * (2 * count + 1),
        scratch_shapes=[
            pltpu.VMEM((plan.lines * 8, LANES), jnp.bfloat16),
            pltpu.SemaphoreType.DMA(()),
            pltpu.SemaphoreType.DMA((QUAD, 2)),
        ],
        compiler_params=params(16),
        name="sent_terms",
    )(*[pltpu.with_memory_space_constraint(x, pltpu.HBM) for x in (blocks, probes)])
    return dict(zip(REDUCE, out[:count])), dict(zip(REDUCE, out[count:-1])), out[-1]


def own_terms(plan, blocks, lhs):
    vmem = pl.BlockSpec(memory_space=pltpu.VMEM)
    return pl.pallas_call(
        functools.partial(own_kernel, plan),
        out_shape=[
            in_vmem((plan.quarter, 8, LANES), jnp.float32),
            in_vmem((plan.quarter * STEP, LANES), jnp.bfloat16),
        ],
        in_specs=[pl.BlockSpec(memory_space=pl.ANY), vmem],
        out_specs=[vmem] * 2,
        scratch_shapes=[pltpu.SemaphoreType.DMA((2,))],
        compiler_params=params(16),
        name="own_terms",
    )(pltpu.with_memory_space_constraint(blocks, pltpu.HBM), *from_vmem(lhs))


def gram_terms(plan, ins):
    row = row_of()
    lane = lane_of()
    sums = [jnp.zeros((8, LANES), jnp.float32) for _ in range(3)]
    for in_ref in ins:
        for t in range(plan.quarter):
            x = in_ref[t]
            for d in range(3):
                y = x if d == 0 else jnp.where(row % 4 + d < 4, roll(x, -d, 0), roll(x, 4 - d, 0))
                sums[d] = sums[d] + x * y
    packed = jnp.zeros((8, LANES), jnp.float32)
    for d in range(3):
        packed = jnp.where(lane == d, jnp.sum(sums[d], axis=1, keepdims=True), packed)
    return packed


def adjoint_kernel(plan, distances, follows, last, *refs):
    count = len(distances)
    ins, kepts, rest = refs[:count], refs[count : 2 * count], refs[2 * count :]
    earlier = rest[0] if follows else None
    acc_ref = rest[-1]
    param = lax.axis_index("param")
    low = row_of() < 4
    even = lane_of() % 2 == 0
    column = lane_of((8, STEP))
    if follows and not last:
        acc_ref[...] = earlier[...]
    else:
        acc_ref[...] = jnp.zeros(acc_ref.shape, jnp.float32)
    for k, in_ref, kept_ref in zip(distances, ins, kepts):
        first = (param & (QUAD - 1) ^ k) * plan.quarter

        def body(t, _, first=first, in_ref=in_ref, kept_ref=kept_ref):
            step = jnp.minimum(first + t, plan.steps - 1)
            line = first_line(plan, step)
            x = in_ref[t]
            y = jnp.where(even, roll(x, -1, 1), -roll(x, 1, 1))
            left = jnp.where(low, x, roll(y, 4, 0))
            right = jnp.where(low, roll(x, 4, 0), y)
            value = jnp.concatenate([left, right], axis=1)
            mine = column + step * STEP < (line + 1) * plan.per_line
            terms = []
            for _ in range(SPLITS):
                term = value.astype(jnp.bfloat16).astype(jnp.float32)
                terms.append(jnp.where(mine, term, 0.0))
                terms.append(jnp.where(mine, 0.0, term))
                value = value - term
            lhs = jnp.concatenate(terms, axis=0).astype(jnp.bfloat16)
            block = kept_ref[pl.ds(pl.multiple_of(t * STEP, STEP), STEP)]
            got = jnp.dot(lhs, block, preferred_element_type=jnp.float32)
            here = sum(got[16 * i : 16 * i + 8] for i in range(SPLITS))
            after = sum(got[16 * i + 8 : 16 * i + 16] for i in range(SPLITS))
            acc_ref[line] = acc_ref[line] + here
            acc_ref[line + 1] = acc_ref[line + 1] + after
            return 0

        lax.fori_loop(0, plan.quarter, body, 0, unroll=True)
    packed = gram_terms(plan, ins)
    if follows:
        packed = packed + earlier[plan.lines]
    if not last:
        acc_ref[plan.lines] = packed
        return
    spot = lax.axis_index("sensor")
    for k, out_ref in enumerate(rest[1:-1]):
        lines = pl.ds((spot ^ k) * plan.shard_lines, plan.shard_lines)
        out_ref[pl.ds(0, plan.shard_lines)] = acc_ref[lines] + earlier[lines]
        out_ref[plan.shard_lines] = packed


def adjoint_terms(plan, distances, pieces, kept, earlier=None, last=False):
    vmem = pl.BlockSpec(memory_space=pltpu.VMEM)
    whole = in_vmem((plan.lines + 1, 8, LANES), jnp.float32)
    shard = in_vmem((plan.shard_lines + 1, 8, LANES), jnp.float32)
    given = [pieces[k] for k in distances] + [kept[k] for k in distances]
    if earlier is not None:
        given.append(earlier)
    return pl.pallas_call(
        functools.partial(adjoint_kernel, plan, distances, earlier is not None, last),
        out_shape=[shard] * plan.shards if last else whole,
        in_specs=[vmem] * len(given),
        out_specs=[vmem] * plan.shards if last else vmem,
        scratch_shapes=[whole] if last else [],
        compiler_params=params(16),
        name="adjoint_last" if last else "adjoint_part",
    )(*from_vmem(*given))


def by_line_kernel(plan, *rest):
    ins, out_ref, flat_ref = rest[:QUAD], rest[QUAD], rest[QUAD + 1]
    me = lax.axis_index("param") & (QUAD - 1)
    lane = lane_of()
    half = LANES // 2
    stay = (row_of() < 4) == (lane < half)
    source = jnp.where(lane < half, 2 * lane, 2 * lane - (LANES - 1))
    for k in range(QUAD):
        first = (me ^ k) * plan.quarter
        for t in range(plan.quarter):
            split = jnp.take_along_axis(ins[k][t], source, axis=1)
            flat_ref[first + t] = jnp.where(stay, split, roll(roll(split, 4, 0), half, 1))
    tiles = -(-plan.group // LANES)
    for line in range(plan.lines):
        tile, shift = divmod(line * plan.group, LANES)
        turned = [roll(flat_ref[tile + i], -shift, 1) for i in range(tiles + 1)]
        for i in range(tiles):
            width = min(LANES, plan.group - i * LANES)
            part = jnp.where(lane < LANES - shift, turned[i], turned[i + 1])
            out_ref[line, :, pl.ds(i * LANES, width)] = part[:, :width]


def sketch_by_line(plan, pieces):
    vmem = pl.BlockSpec(memory_space=pltpu.VMEM)
    return pl.pallas_call(
        functools.partial(by_line_kernel, plan),
        out_shape=in_vmem((plan.lines, 8, plan.group), jnp.float32),
        in_specs=[vmem] * QUAD,
        out_specs=vmem,
        scratch_shapes=[pltpu.VMEM((QUAD * plan.quarter + 2, 8, LANES), jnp.float32)],
        compiler_params=params(16),
        name="sketch_by_line",
    )(*from_vmem(*pieces))


def inverse_rows(plan, packed):
    row = row_of()
    lane = lane_of()
    packed = packed + roll(packed, 4, 0)
    entry = {}
    for d in range(3):
        for a in range(PROBES):
            b = (a + d) % PROBES
            if (max(a, b), min(a, b)) not in entry:
                chosen = jnp.where((row == a) & (lane == d), packed, 0.0)
                whole = jnp.sum(jnp.sum(chosen, axis=1, keepdims=True), axis=0, keepdims=True)
                entry[max(a, b), min(a, b)] = jnp.broadcast_to(whole, (8, LANES)) / plan.total
    low = {}
    inv = {}
    for j in range(PROBES):
        rest = entry[j, j]
        for m in range(j):
            rest = rest - low[j, m] * low[j, m]
        low[j, j] = jnp.sqrt(rest)
        inv[j, j] = 1.0 / low[j, j]
        for i in range(j + 1, PROBES):
            rest = entry[i, j]
            for m in range(j):
                rest = rest - low[i, m] * low[j, m]
            low[i, j] = rest * inv[j, j]
    for i in range(PROBES):
        for j in range(i):
            total = sum(low[i, m] * inv[m, j] for m in range(j, i))
            inv[i, j] = -total * inv[i, i]
    rows = []
    for d in range(PROBES):
        value = jnp.zeros((8, LANES), jnp.float32)
        for a in range(d, PROBES):
            value = jnp.where(row % 4 == a, inv[a, a - d], value)
        rows.append(value)
    return rows


def final_kernel(plan, sketch_ref, *rest):
    ins, (basis_out, coeffs_out, basis_ref, coeffs_ref, sems) = rest[: plan.shards], rest[plan.shards :]
    packed = sum(ref[plan.shard_lines] for ref in ins)
    rows = inverse_rows(plan, packed)

    def scaled(x):
        width = x.shape[1]
        return sum((rows[d][:, :width] * (roll(x, d, 0) if d else x)) for d in range(PROBES))

    copies = []
    for at in range(PIECES):
        low, high = at * plan.lines // PIECES, (at + 1) * plan.lines // PIECES
        for line in range(low, high):
            for start in range(0, plan.group, LANES):
                width = min(LANES, plan.group - start)
                value = scaled(sketch_ref[line, :, pl.ds(start, width)])
                for part in range(2):
                    basis_ref[line, part, :, pl.ds(start, width)] = value[4 * part : 4 * part + 4]
        made = pl.ds(low, high - low)
        copies.append(pltpu.make_async_copy(basis_ref.at[made], basis_out.at[made], sems.at[at]))
        copies[-1].start()
    for pair in range(plan.shard_lines // 2):
        two = [scaled(sum(ref[2 * pair + i] for ref in ins)) for i in range(2)]
        coeffs_ref[pl.ds(16 * pair, 16)] = jnp.concatenate(two, axis=0).astype(jnp.bfloat16)
    copies.append(pltpu.make_async_copy(coeffs_ref, coeffs_out, sems.at[PIECES]))
    copies[-1].start()
    for copy in copies:
        copy.wait()


def finish(plan, sketch, pieces):
    vmem = pl.BlockSpec(memory_space=pltpu.VMEM)
    basis = (plan.lines, 2, PROBES, plan.group)
    coeffs = (plan.shard_lines * 8, LANES)
    return pl.pallas_call(
        functools.partial(final_kernel, plan),
        out_shape=[jax.ShapeDtypeStruct(basis, jnp.float32), jax.ShapeDtypeStruct(coeffs, jnp.bfloat16)],
        in_specs=[vmem] * (1 + plan.shards),
        out_specs=[pl.BlockSpec(memory_space=pltpu.HBM)] * 2,
        scratch_shapes=[
            pltpu.VMEM(basis, jnp.float32),
            pltpu.VMEM(coeffs, jnp.bfloat16),
            pltpu.SemaphoreType.DMA((PIECES + 1,)),
        ],
        compiler_params=params(16),
        name="finish",
    )(*from_vmem(sketch, *pieces))


def trade(x, axis, size, k):
    return lax.ppermute(x, axis, [(i, i ^ k) for i in range(size)])


def sketch_and_adjoint(param, sensor, blocks, probes):
    lines, parts, group, nodes = blocks.shape
    plan = Plan(lines, parts, group, nodes, sensor)
    flat_blocks = blocks.transpose(0, 2, 1, 3).reshape(plan.rows, nodes)
    flat_probes = probes.reshape(lines * parts * PROBES, nodes)
    terms, kept, lhs = sketch_terms(plan, flat_blocks, flat_probes)
    total, kept[0] = own_terms(plan, flat_blocks, lhs)
    for k in REDUCE:
        total = total + trade(terms[k], "param", param, k)
    span = QUAD
    while span * 2 < param:
        total = total + trade(total, "param", param, span)
        span *= 2
    sums = [total] + ([trade(total, "param", param, span)] if span < param else [])
    own = sum(sums)
    pieces = [own] + [trade(own, "param", param, k) for k in range(1, QUAD)]
    adjoint = adjoint_terms(plan, (0,), pieces, kept)
    adjoint = adjoint_terms(plan, GATHER[:1], pieces, kept, adjoint)
    adjoint = adjoint_terms(plan, GATHER[1:-1], pieces, kept, adjoint)
    adjoint = adjoint_terms(plan, GATHER[-1:], pieces, kept, adjoint, True)
    gathered = [adjoint[0]] + [trade(adjoint[k], "sensor", sensor, k) for k in range(1, sensor)]
    sketch = sketch_by_line(plan, pieces)
    basis, coeffs = finish(plan, sketch, gathered)
    return basis, coeffs.reshape(plan.shard_lines, parts, PROBES, nodes)


def on_device(param, sensor, blocks, probes):
    return sketch_and_adjoint(param, sensor, blocks, probes)


def solution(mesh):
    param, sensor = mesh.shape["param"], mesh.shape["sensor"]
    assert param % QUAD == 0 and param & (param - 1) == 0 and sensor & (sensor - 1) == 0
    placed = (P(None, None, "sensor", "param"), P(None, None, None, "param"))
    return jax.shard_map(
        functools.partial(on_device, param, sensor),
        mesh=mesh,
        in_specs=placed,
        out_specs=(P(None, None, None, "sensor"), P("sensor", None, None, "param")),
        check_vma=False,
    )
```
